16 devices in a mesh: data: 2 (over y, z), tp: 8 (over x, core).
Axes of the slice: x: 4, y: 2, z: 1, core: 2. Of those that a mesh axis runs over, the one named last changes fastest.
The devices are a block of a 4x4x8 slice.
Arguments:
- x: bfloat16 [16384, 8192], P('data', 'tp'), parts along dimension 0
- w: bfloat16 [8192, 2048], P('tp')
- r: bfloat16 [16384, 2048], P('data'), parts along dimension 0
- g: bfloat16 [2048], replicated
Outputs:
- output: bfloat16 [16384, 2048], P('data'), parts along dimension 0
There are 2 independent parts. The reference program is written for one: setup_inputs(seed, part) draws one part's arguments, and reference() takes and returns one part's arrays. A program takes and returns all parts, laid end to end along the dimension named above; an argument that names none is the same for every part.
All inputs are finite; a program needn't handle non-finite values.
Results may differ from the reference program's by a relative error of at most 0.0108205.
Values are sent between devices in bfloat16 or wider.
A program may use at most 768 MiB of HBM per device.

```python
import jax
import jax.numpy as jnp
from jax import lax

T = 8192
H = 2048
F = 8192
EPS = 1e-6


def setup_inputs(seed: int = 0, part: int = 0) -> dict:
    kp = jax.random.fold_in(jax.random.key(seed), part)
    kx, kr = jax.random.split(kp)
    kw, kg = jax.random.split(jax.random.key(seed + 1))
    x = jax.random.normal(kx, (T, F), jnp.float32).astype(jnp.bfloat16)
    w = (jax.random.normal(kw, (F, H), jnp.float32) * (F ** -0.5)).astype(jnp.bfloat16)
    r = jax.random.normal(kr, (T, H), jnp.float32).astype(jnp.bfloat16)
    g = jax.random.uniform(kg, (H,), jnp.float32, 0.5, 1.5).astype(jnp.bfloat16)
    return {"x": x, "w": w, "r": r, "g": g}


def reference(x, w, r, g):
    y = jnp.dot(x, w, preferred_element_type=jnp.float32).astype(jnp.bfloat16)
    a = r.astype(jnp.float32) + y.astype(jnp.float32)
    ms = jnp.mean(a * a, axis=-1, keepdims=True)
    z = a * lax.rsqrt(ms + EPS) * g.astype(jnp.float32)
    return z.astype(jnp.bfloat16)
```

```python
import functools

import jax
import jax.numpy as jnp
from jax import lax
from jax.experimental import pallas as pl
from jax.experimental.pallas import tpu as pltpu
from jax.sharding import PartitionSpec as P

EPS = 1e-6
MESH = pl.DeviceIdType.MESH
CHIPS = 4
NW = 4
NC = 4
NS = 2
SLOTS = 4


def ring_kernel(
    x, w, r, g, z,
    w_own, w_par, xt, xp, far, near1, stage, rt,
    w_sem, xt_sem, rt_sem,
    wx_send, wx_recv, xp_send, xp_recv,
    st_send, far_recv, near_recv,
    own_send, ag_recv, fwd_send, fwd_recv, d_send, d_recv,
):
    me = lax.axis_index("tp")
    k = lax.rem(me, 2)
    c = lax.div(me, 2)
    chip = lambda d: lax.rem(c + d, CHIPS)
    mine = lambda d: chip(d) * 2 + k
    other = lambda d: chip(d) * 2 + 1 - k
    partner = c * 2 + 1 - k
    to = (mine(1), mine(3))
    NEAR = (1, 3)
    rw, kd = x.shape[3], x.shape[4]
    hid = w.shape[1]
    cw = hid // NC
    sr = rw // NS

    def remote(src, dst, ssem, rsem, dev):
        return pltpu.make_async_remote_copy(
            src_ref=src, dst_ref=dst, send_sem=ssem, recv_sem=rsem,
            device_id={"tp": dev}, device_id_type=MESH,
        )

    def cols(j):
        return pl.ds(pl.multiple_of(j * cw, cw), cw)

    def w_local(j):
        return pltpu.make_async_copy(w.at[:, cols(j)], w_own.at[j], w_sem.at[j])

    def w_remote(j):
        return remote(w.at[:, cols(j)], w_par.at[j], wx_send.at[j], wx_recv.at[j], partner)

    def x_local(t, d, wv):
        return pltpu.make_async_copy(x.at[mine(d), :, wv], xt.at[t], xt_sem.at[t])

    def x_remote(e, d, wv):
        return remote(
            x.at[other(d), :, wv], xp.at[e, wv], xp_send.at[e, wv], xp_recv.at[e, wv], partner
        )

    def r_local(wv, h):
        return pltpu.make_async_copy(r.at[mine(0), h, wv], rt.at[h], rt_sem.at[h])

    def far_copy(D, slot, wv, j):
        return remote(
            stage.at[D, slot, 0], far.at[D, wv, j],
            st_send.at[D, slot], far_recv.at[D, wv, j], to[D],
        )

    def near_copy(D, slot, wv, j):
        if D == 0:
            dst = z.at[to[0], :, wv, :, cols(j)]
        else:
            dst = near1.at[wv, :, :, cols(j)]
        return remote(stage.at[D, slot], dst, st_send.at[D, slot], near_recv.at[D, wv, j], to[D])

    def rows(s):
        return pl.ds(pl.multiple_of(s * sr, sr), sr)

    def zrow(b, wv, h, s):
        return z.at[b, h, wv, rows(s)]

    def own_copy(D, wv, h, s):
        v = zrow(mine(0), wv, h, s)
        return remote(v, v, own_send.at[D, wv, h, s], ag_recv.at[D, wv, h, s], to[D])

    def ag_landed(D, wv, h, s):
        v = zrow(mine(4 - NEAR[D]), wv, h, s)
        return remote(v, v, own_send.at[D, wv, h, s], ag_recv.at[D, wv, h, s], to[D])

    def fwd_copy(D, wv, s):
        v = zrow(mine(4 - NEAR[D]), wv, D, s)
        return remote(v, v, fwd_send.at[D, wv, s], fwd_recv.at[D, wv, s], to[D])

    def fwd_landed(D, wv, s):
        v = zrow(mine(2), wv, D, s)
        return remote(v, v, fwd_send.at[D, wv, s], fwd_recv.at[D, wv, s], to[D])

    def d2d(e, d, wv, h, s):
        v = zrow(mine(d), wv, h, s)
        return remote(v, v, d_send.at[e, wv, h, s], d_recv.at[e, wv, h, s], partner)

    def product(t, e, wv, j):
        a = xt[t].reshape(2 * rw, kd)
        b = xp[e, wv].reshape(2 * rw, kd)
        acc = jnp.dot(a, w_own[j], preferred_element_type=jnp.float32)
        return acc + jnp.dot(b, w_par[j], preferred_element_type=jnp.float32)

    barrier = pltpu.get_barrier_semaphore()
    for dev in (partner, to[0], to[1]):
        pl.semaphore_signal(barrier, inc=1, device_id={"tp": dev}, device_id_type=MESH)
    pl.semaphore_wait(barrier, 3)

    x_local(0, 2, 0).start()
    x_remote(0, 2, 0).start()
    for j in range(NC):
        w_local(j).start()
        w_remote(j).start()
    for wv in range(1, NW):
        x_local(wv, 2, wv).start()
        x_remote(0, 2, wv).start()
    for wv in range(NW):
        for D in range(2):
            x_remote(1 + D, NEAR[D], wv).start()
    for wv in range(NW):
        x_remote(3, 0, wv).start()
    for h in range(2):
        r_local(0, h).start()

    @pl.loop(0, NW)
    def _(wv):
        x_local(wv, 2, wv).wait()
        x_remote(0, 2, wv).wait_recv()

        @pl.loop(0, NC)
        def _(j):
            n = wv * NC + j
            slot = lax.rem(n, SLOTS)

            @pl.when(wv == 0)
            def _():
                w_local(j).wait()
                w_remote(j).wait_recv()

            acc = product(wv, 0, wv, j)
            for D in range(2):

                @pl.when(n >= SLOTS)
                def _():
                    far_copy(D, slot, wv, j).wait_send()

                stage[D, slot, 0] = acc[D * rw : (D + 1) * rw].astype(jnp.bfloat16)
                far_copy(D, slot, wv, j).start()

        D = lax.rem(wv, 2)
        x_local(wv, 1 + 2 * D, lax.div(wv, 2)).start()

    @pl.loop(0, NW)
    def _(wv):
        t0 = lax.rem(2 * wv, 4)
        for D in range(2):
            x_local(t0 + D, NEAR[D], wv).wait()
            x_remote(1 + D, NEAR[D], wv).wait_recv()

        @pl.loop(0, NC)
        def _(j):
            n = wv * NC + j
            slot = lax.rem(n, SLOTS)
            for D in range(2):
                acc = product(t0 + D, 1 + D, wv, j)

                @pl.when(n < SLOTS)
                def _():
                    far_copy(D, slot, wv, j).wait_send()

                @pl.when(n >= SLOTS)
                def _():
                    near_copy(D, slot, wv, j).wait_send()

                far_copy(D, slot, wv, j).wait_recv()
                for h in range(2):
                    part = acc[h * rw : (h + 1) * rw]
                    if h == D:
                        part = part + far[D, wv, j].astype(jnp.float32)
                    stage[D, slot, h] = part.astype(jnp.bfloat16)
                near_copy(D, slot, wv, j).start()

        for D in range(2):

            @pl.when(wv < 2)
            def _():
                x_local(t0 + D, NEAR[D], wv + 2).start()

            @pl.when(wv >= 2)
            def _():
                x_local(t0 + D, 0, 2 * (wv - 2) + D).start()

    @pl.loop(0, NW)
    def _(wv):
        x_local(wv, 0, wv).wait()
        x_remote(3, 0, wv).wait_recv()

        @pl.loop(0, NC)
        def _(j):
            acc = product(wv, 3, wv, j)
            for D in range(2):
                near_copy(D, 0, wv, j).wait_recv()
            for h in range(2):
                y = acc[h * rw : (h + 1) * rw]
                y = y + z[mine(0), h, wv, :, cols(j)].astype(jnp.float32)
                y = y + near1[wv, h, :, cols(j)].astype(jnp.float32)
                z[mine(0), h, wv, :, cols(j)] = y.astype(jnp.bfloat16)

        for h in range(2):
            r_local(wv, h).wait()

            @pl.loop(0, NS)
            def _(s):
                @pl.loop(0, sr // 16)
                def _(i):
                    q = pl.ds(pl.multiple_of(s * sr + i * 16, 16), 16)
                    a = rt[h, q].astype(jnp.float32) + z[mine(0), h, wv, q].astype(jnp.float32)
                    ms = jnp.mean(a * a, axis=-1, keepdims=True)
                    zz = a * lax.rsqrt(ms + EPS) * g[...].astype(jnp.float32)
                    z[mine(0), h, wv, q] = zz.astype(jnp.bfloat16)

                for D in range(2):
                    own_copy(D, wv, h, s).start()
                d2d(0, 0, wv, h, s).start()

            @pl.when(wv < NW - 1)
            def _():
                r_local(wv + 1, h).start()

    @pl.loop(0, NW)
    def _(wv):
        for h in range(2):

            @pl.loop(0, NS)
            def _(s):
                for D in range(2):
                    ag_landed(D, wv, h, s).wait_recv()
                    if h == D:
                        fwd_copy(D, wv, s).start()
                    d2d(1 + D, 4 - NEAR[D], wv, h, s).start()

    @pl.loop(0, NW)
    def _(wv):
        @pl.loop(0, NS)
        def _(s):
            for D in range(2):
                fwd_landed(D, wv, s).wait_recv()
                d2d(3, 2, wv, D, s).start()

    @pl.loop(0, SLOTS)
    def _(slot):
        for D in range(2):
            near_copy(D, slot, 0, 0).wait_send()

    @pl.loop(0, NW)
    def _(wv):
        w_remote(wv).wait_send()
        for e, d in ((0, 2), (1, 1), (2, 3), (3, 0)):
            x_remote(e, d, wv).wait_send()

        @pl.loop(0, NS)
        def _(s):
            for D in range(2):
                for h in range(2):
                    own_copy(D, wv, h, s).wait_send()
                fwd_copy(D, wv, s).wait_send()
            for e, d in ((0, 0), (1, 3), (2, 1), (3, 2)):
                for h in range(2):
                    d2d(e, d, wv, h, s).wait_send()
                    d2d(e, d, wv, h, s).wait_recv()


def store_kernel(z, o, sem):
    n = z.shape[0]
    for i in range(n):
        pltpu.make_async_copy(z.at[i], o.at[i], sem.at[i]).start()
    for i in range(n):
        pltpu.make_async_copy(z.at[i], o.at[i], sem.at[i]).wait()


def solution(mesh):
    tp = mesh.shape["tp"]

    def local(x, w, r, g):
        t, kd = x.shape
        hid = w.shape[1]
        half = t // tp // 2
        rw, cw = half // NW, hid // NC
        x5 = x.reshape(tp, 2, NW, rw, kd)
        r5 = r.reshape(tp, 2, NW, rw, hid)
        dma = pltpu.SemaphoreType.DMA
        bf = jnp.bfloat16
        any_spec = pl.BlockSpec(memory_space=pl.ANY)
        z = pl.pallas_call(
            ring_kernel,
            name="ring",
            out_shape=pltpu.VMEM((tp, 2, NW, rw, hid), bf),
            in_specs=[any_spec, any_spec, any_spec, pl.BlockSpec(memory_space=pltpu.VMEM)],
            out_specs=pl.BlockSpec(memory_space=pltpu.VMEM),
            scratch_shapes=[
                pltpu.VMEM((NC, kd, cw), bf),
                pltpu.VMEM((NC, kd, cw), bf),
                pltpu.VMEM((4, 2, rw, kd), bf),
                pltpu.VMEM((4, NW, 2, rw, kd), bf),
                pltpu.VMEM((2, NW, NC, rw, cw), bf),
                pltpu.VMEM((NW, 2, rw, hid), bf),
                pltpu.VMEM((2, SLOTS, 2, rw, cw), bf),
                pltpu.VMEM((2, rw, hid), bf),
                dma((NC,)), dma((4,)), dma((2,)),
                dma((NC,)), dma((NC,)), dma((4, NW)), dma((4, NW)),
                dma((2, SLOTS)), dma((2, NW, NC)), dma((2, NW, NC)),
                dma((2, NW, 2, NS)), dma((2, NW, 2, NS)), dma((2, NW, NS)), dma((2, NW, NS)),
                dma((4, NW, 2, NS)), dma((4, NW, 2, NS)),
            ],
            compiler_params=pltpu.CompilerParams(
                collective_id=0, has_side_effects=True, vmem_limit_bytes=33000000
            ),
        )(x5, w, r5, g.reshape(1, hid))
        out = pl.pallas_call(
            store_kernel,
            name="store",
            out_shape=jax.ShapeDtypeStruct(z.shape, bf),
            in_specs=[pl.BlockSpec(memory_space=pltpu.VMEM)],
            out_specs=any_spec,
            scratch_shapes=[dma((tp,))],
            compiler_params=pltpu.CompilerParams(vmem_limit_bytes=1 << 20),
        )(z)
        return out.reshape(t, hid)

    return jax.shard_map(
        local,
        mesh=mesh,
        in_specs=(P("data", "tp"), P("tp", None), P("data", None), P(None)),
        out_specs=P("data", None),
        check_vma=False,
    )
```

```python
import functools

import jax
import jax.numpy as jnp
from jax import lax
from jax.experimental import pallas as pl
from jax.experimental.pallas import tpu as pltpu
from jax.sharding import PartitionSpec as P

EPS = 1e-6
MESH = pl.DeviceIdType.MESH
CHIPS = 4
NW = 4
NC = 4
NS = 2
SLOTS = 4


def ring_kernel(
    x, w, r, g, z,
    gv, w_own, w_par, xt, xp, far, near1, stage, rt,
    g_sem, w_sem, xt_sem, rt_sem,
    wx_send, wx_recv, xp_send, xp_recv,
    st_send, far_recv, near_recv,
    own_send, ag_recv, fwd_send, fwd_recv, d_send, d_recv,
):
    me = lax.axis_index("tp")
    k = lax.rem(me, 2)
    c = lax.div(me, 2)
    chip = lambda d: lax.rem(c + d, CHIPS)
    mine = lambda d: chip(d) * 2 + k
    other = lambda d: chip(d) * 2 + 1 - k
    partner = c * 2 + 1 - k
    to = (mine(1), mine(3))
    NEAR = (1, 3)
    rw, kd = x.shape[3], x.shape[4]
    hid = w.shape[1]
    cw = hid // NC
    sr = rw // NS

    def remote(src, dst, ssem, rsem, dev):
        return pltpu.make_async_remote_copy(
            src_ref=src, dst_ref=dst, send_sem=ssem, recv_sem=rsem,
            device_id={"tp": dev}, device_id_type=MESH,
        )

    def cols(j):
        return pl.ds(pl.multiple_of(j * cw, cw), cw)

    def w_local(j):
        return pltpu.make_async_copy(w.at[:, cols(j)], w_own.at[j], w_sem.at[j])

    def w_remote(j):
        return remote(w.at[:, cols(j)], w_par.at[j], wx_send.at[j], wx_recv.at[j], partner)

    def x_local(t, d, wv):
        return pltpu.make_async_copy(x.at[mine(d), :, wv], xt.at[t], xt_sem.at[t])

    def x_remote(e, d, wv):
        return remote(
            x.at[other(d), :, wv], xp.at[e, wv], xp_send.at[e, wv], xp_recv.at[e, wv], partner
        )

    def r_local(wv, h):
        return pltpu.make_async_copy(r.at[mine(0), h, wv], rt.at[h], rt_sem.at[h])

    def far_copy(D, slot, wv, j):
        return remote(
            stage.at[D, slot, 0], far.at[D, wv, j],
            st_send.at[D, slot], far_recv.at[D, wv, j], to[D],
        )

    def near_copy(D, slot, wv, j):
        if D == 0:
            dst = z.at[to[0], :, wv, :, cols(j)]
        else:
            dst = near1.at[wv, :, :, cols(j)]
        return remote(stage.at[D, slot], dst, st_send.at[D, slot], near_recv.at[D, wv, j], to[D])

    def rows(s):
        return pl.ds(pl.multiple_of(s * sr, sr), sr)

    def zrow(b, wv, h, s):
        return z.at[b, h, wv, rows(s)]

    def own_copy(D, wv, h, s):
        v = zrow(mine(0), wv, h, s)
        return remote(v, v, own_send.at[D, wv, h, s], ag_recv.at[D, wv, h, s], to[D])

    def ag_landed(D, wv, h, s):
        v = zrow(mine(4 - NEAR[D]), wv, h, s)
        return remote(v, v, own_send.at[D, wv, h, s], ag_recv.at[D, wv, h, s], to[D])

    def fwd_copy(D, wv, s):
        v = zrow(mine(4 - NEAR[D]), wv, D, s)
        return remote(v, v, fwd_send.at[D, wv, s], fwd_recv.at[D, wv, s], to[D])

    def fwd_landed(D, wv, s):
        v = zrow(mine(2), wv, D, s)
        return remote(v, v, fwd_send.at[D, wv, s], fwd_recv.at[D, wv, s], to[D])

    def d2d(d, wv, h, s):
        v = zrow(mine(d), wv, h, s)
        return remote(v, v, d_send.at[0], d_recv.at[0], partner)

    def product(t, e, wv, j):
        a = xt[t].reshape(2 * rw, kd)
        b = xp[e, wv].reshape(2 * rw, kd)
        acc = jnp.dot(a, w_own[j], preferred_element_type=jnp.float32)
        return acc + jnp.dot(b, w_par[j], preferred_element_type=jnp.float32)

    barrier = pltpu.get_barrier_semaphore()
    for dev in (partner, to[0], to[1]):
        pl.semaphore_signal(barrier, inc=1, device_id={"tp": dev}, device_id_type=MESH)
    x_local(0, 2, 0).start()
    for j in range(NC):
        w_local(j).start()
    for wv in range(1, NW):
        x_local(wv, 2, wv).start()
    for h in range(2):
        r_local(0, h).start()
    pltpu.make_async_copy(g, gv, g_sem).start()
    pl.semaphore_wait(barrier, 3)

    x_remote(0, 2, 0).start()
    for j in range(NC):
        w_remote(j).start()
    for wv in range(1, NW):
        x_remote(0, 2, wv).start()
    for wv in range(NW):
        for D in range(2):
            x_remote(1 + D, NEAR[D], wv).start()
    for wv in range(NW):
        x_remote(3, 0, wv).start()

    @pl.loop(0, NW)
    def _(wv):
        x_local(wv, 2, wv).wait()
        x_remote(0, 2, wv).wait_recv()

        @pl.loop(0, NC)
        def _(j):
            n = wv * NC + j
            slot = lax.rem(n, SLOTS)

            @pl.when(wv == 0)
            def _():
                w_local(j).wait()
                w_remote(j).wait_recv()

            acc = product(wv, 0, wv, j)
            for D in range(2):

                @pl.when(n >= SLOTS)
                def _():
                    far_copy(D, slot, wv, j).wait_send()

                stage[D, slot, 0] = acc[D * rw : (D + 1) * rw].astype(jnp.bfloat16)
                far_copy(D, slot, wv, j).start()

        D = lax.rem(wv, 2)
        x_local(wv, 1 + 2 * D, lax.div(wv, 2)).start()

    @pl.loop(0, NW)
    def _(wv):
        t0 = lax.rem(2 * wv, 4)
        for D in range(2):
            x_local(t0 + D, NEAR[D], wv).wait()
            x_remote(1 + D, NEAR[D], wv).wait_recv()

        @pl.loop(0, NC)
        def _(j):
            n = wv * NC + j
            slot = lax.rem(n, SLOTS)
            for D in range(2):
                acc = product(t0 + D, 1 + D, wv, j)

                @pl.when(n < SLOTS)
                def _():
                    far_copy(D, slot, wv, j).wait_send()

                @pl.when(n >= SLOTS)
                def _():
                    near_copy(D, slot, wv, j).wait_send()

                far_copy(D, slot, wv, j).wait_recv()
                for h in range(2):
                    part = acc[h * rw : (h + 1) * rw]
                    if h == D:
                        part = part + far[D, wv, j].astype(jnp.float32)
                    stage[D, slot, h] = part.astype(jnp.bfloat16)
                near_copy(D, slot, wv, j).start()

        for D in range(2):

            @pl.when(wv < 2)
            def _():
                x_local(t0 + D, NEAR[D], wv + 2).start()

            @pl.when(wv >= 2)
            def _():
                x_local(t0 + D, 0, 2 * (wv - 2) + D).start()

    pltpu.make_async_copy(g, gv, g_sem).wait()
    gain = gv[...].astype(jnp.float32).reshape(1, hid)

    @pl.loop(0, NW)
    def _(wv):
        x_local(wv, 0, wv).wait()
        x_remote(3, 0, wv).wait_recv()

        @pl.loop(0, NC)
        def _(j):
            acc = product(wv, 3, wv, j)
            for D in range(2):
                near_copy(D, 0, wv, j).wait_recv()
            for h in range(2):
                y = acc[h * rw : (h + 1) * rw]
                y = y + z[mine(0), h, wv, :, cols(j)].astype(jnp.float32)
                y = y + near1[wv, h, :, cols(j)].astype(jnp.float32)
                z[mine(0), h, wv, :, cols(j)] = y.astype(jnp.bfloat16)

        for h in range(2):
            r_local(wv, h).wait()

            @pl.loop(0, NS)
            def _(s):
                @pl.loop(0, sr // 16)
                def _(i):
                    q = pl.ds(pl.multiple_of(s * sr + i * 16, 16), 16)
                    a = rt[h, q].astype(jnp.float32) + z[mine(0), h, wv, q].astype(jnp.float32)
                    ms = jnp.mean(a * a, axis=-1, keepdims=True)
                    zz = a * lax.rsqrt(ms + EPS) * gain
                    z[mine(0), h, wv, q] = zz.astype(jnp.bfloat16)

                for D in range(2):
                    own_copy(D, wv, h, s).start()
                d2d(0, wv, h, s).start()

            @pl.when(wv < NW - 1)
            def _():
                r_local(wv + 1, h).start()

    @pl.loop(0, NW)
    def _(wv):
        for h in range(2):

            @pl.loop(0, NS)
            def _(s):
                for D in range(2):
                    ag_landed(D, wv, h, s).wait_recv()
                    if h == D:
                        fwd_copy(D, wv, s).start()
                    d2d(4 - NEAR[D], wv, h, s).start()

    @pl.loop(0, SLOTS)
    def _(slot):
        for D in range(2):
            near_copy(D, slot, 0, 0).wait_send()

    @pl.loop(0, NW)
    def _(wv):
        for e, d in ((0, 2), (1, 1), (2, 3), (3, 0)):
            x_remote(e, d, wv).wait_send()

        @pl.loop(0, NS)
        def _(s):
            for D in range(2):
                for h in range(2):
                    own_copy(D, wv, h, s).wait_send()

    @pl.loop(0, NC)
    def _(j):
        w_remote(j).wait_send()

    @pl.loop(0, NW)
    def _(wv):
        @pl.loop(0, NS)
        def _(s):
            for D in range(2):
                fwd_landed(D, wv, s).wait_recv()
                d2d(2, wv, D, s).start()
                fwd_copy(D, wv, s).wait_send()

    every = z.at[pl.ds(0, CHIPS)]
    d2d_all = remote(every, every, d_send.at[0], d_recv.at[0], partner)
    d2d_all.wait_send()
    d2d_all.wait_recv()


def store_kernel(z, o, sem):
    n = z.shape[0]
    for i in range(n):
        pltpu.make_async_copy(z.at[i], o.at[i], sem.at[i]).start()
    for i in range(n):
        pltpu.make_async_copy(z.at[i], o.at[i], sem.at[i]).wait()


def solution(mesh):
    tp = mesh.shape["tp"]

    def local(x, w, r, g):
        t, kd = x.shape
        hid = w.shape[1]
        half = t // tp // 2
        rw, cw = half // NW, hid // NC
        x5 = x.reshape(tp, 2, NW, rw, kd)
        r5 = r.reshape(tp, 2, NW, rw, hid)
        dma = pltpu.SemaphoreType.DMA
        bf = jnp.bfloat16
        any_spec = pl.BlockSpec(memory_space=pl.ANY)
        z = pl.pallas_call(
            ring_kernel,
            name="ring",
            out_shape=pltpu.VMEM((tp, 2, NW, rw, hid), bf),
            in_specs=[any_spec] * 4,
            out_specs=pl.BlockSpec(memory_space=pltpu.VMEM),
            scratch_shapes=[
                pltpu.VMEM((hid,), bf),
                pltpu.VMEM((NC, kd, cw), bf),
                pltpu.VMEM((NC, kd, cw), bf),
                pltpu.VMEM((4, 2, rw, kd), bf),
                pltpu.VMEM((4, NW, 2, rw, kd), bf),
                pltpu.VMEM((2, NW, NC, rw, cw), bf),
                pltpu.VMEM((NW, 2, rw, hid), bf),
                pltpu.VMEM((2, SLOTS, 2, rw, cw), bf),
                pltpu.VMEM((2, rw, hid), bf),
                dma, dma((NC,)), dma((4,)), dma((2,)),
                dma((NC,)), dma((NC,)), dma((4, NW)), dma((4, NW)),
                dma((2, SLOTS)), dma((2, NW, NC)), dma((2, NW, NC)),
                dma((2, NW, 2, NS)), dma((2, NW, 2, NS)), dma((2, NW, NS)), dma((2, NW, NS)),
                dma((1,)), dma((1,)),
            ],
            compiler_params=pltpu.CompilerParams(
                collective_id=0, has_side_effects=True, vmem_limit_bytes=33000000
            ),
        )(x5, w, r5, g)
        out = pl.pallas_call(
            store_kernel,
            name="store",
            out_shape=jax.ShapeDtypeStruct(z.shape, bf),
            in_specs=[pl.BlockSpec(memory_space=pltpu.VMEM)],
            out_specs=any_spec,
            scratch_shapes=[dma((tp,))],
            compiler_params=pltpu.CompilerParams(vmem_limit_bytes=1 << 20),
        )(z)
        return out.reshape(t, hid)

    return jax.shard_map(
        local,
        mesh=mesh,
        in_specs=(P("data", "tp"), P("tp", None), P("data", None), P(None)),
        out_specs=P("data", None),
        check_vma=False,
    )
```

```python
import jax
import jax.numpy as jnp
from jax import lax
from jax.experimental import pallas as pl
from jax.experimental.pallas import tpu as pltpu
from jax.sharding import PartitionSpec as P

EPS = 1e-6
MESH = pl.DeviceIdType.MESH
CHIPS = 4
NW = 4
NC = 4
FS = 2
SLOTS = 4
NEAR = (1, 3)


def ring_kernel(
    x, w, r, g, z, late, last,
    gv, w_own, w_par, xt, xp, pre, far, near1, stage, rt,
    g_sem, w_sem, xt_sem, rt_sem, late_sem,
    wx_send, wx_recv, xp_send, xp_recv, pre_send, pre_recv,
    st_send, far_recv, near_recv,
    own_send, ag_recv, fwd_send, fwd_recv, d_send, d_recv,
):
    me = lax.axis_index("tp")
    k = lax.rem(me, 2)
    c = lax.div(me, 2)
    chip = lambda d: lax.rem(c + d, CHIPS)
    mine = lambda d: chip(d) * 2 + k
    other = lambda d: chip(d) * 2 + 1 - k
    partner = c * 2 + 1 - k
    to = (mine(1), mine(3))
    rw, kd = x.shape[3], x.shape[4]
    hid = w.shape[1]
    cw = hid // NC
    fr = rw // FS
    bf = jnp.bfloat16

    def remote(src, dst, ssem, rsem, dev):
        return pltpu.make_async_remote_copy(
            src_ref=src, dst_ref=dst, send_sem=ssem, recv_sem=rsem,
            device_id={"tp": dev}, device_id_type=MESH,
        )

    def cols(j):
        return pl.ds(pl.multiple_of(j * cw, cw), cw)

    def w_local(j):
        return pltpu.make_async_copy(w.at[:, cols(j)], w_own.at[j], w_sem.at[j])

    def w_remote(j):
        return remote(w.at[:, cols(j)], w_par.at[j], wx_send, wx_recv.at[j], partner)

    def x_local(t, b, wv):
        return pltpu.make_async_copy(x.at[b, :, wv], xt.at[t], xt_sem.at[t])

    def x_remote(e, d, wv):
        q = wv - 1 if e == 0 else (NW - 1 if e < 3 else NW)
        return remote(x.at[other(d), :, wv], xp.at[e * NW + wv - 1], xp_send, xp_recv.at[q], partner)

    def x_landed(first, n, q):
        v = xp.at[pl.ds(first, n)]
        return remote(v, v, xp_send, xp_recv.at[q], partner)

    def pre_copy(j):
        return remote(stage.at[:, j, 1], pre.at[j], pre_send, pre_recv.at[j], partner)

    def r_local(wv, h):
        return pltpu.make_async_copy(r.at[mine(0), h, wv], rt.at[h], rt_sem.at[h])

    def far_copy(D, slot, wv, j):
        return remote(
            stage.at[D, slot, 0], far.at[D, wv, j],
            st_send.at[D, slot], far_recv.at[D, wv], to[D],
        )

    def far_landed(D, wv):
        v = far.at[D, wv]
        return remote(v, v, st_send.at[D, 0], far_recv.at[D, wv], to[D])

    def near_copy(D, slot, wv, j):
        dst = z.at[to[0], :, wv, :, cols(j)] if D == 0 else near1.at[wv, :, :, cols(j)]
        return remote(stage.at[D, slot], dst, st_send.at[D, slot], near_recv.at[D, wv], to[D])

    def near_landed(D, wv):
        v = z.at[mine(0), :, wv] if D == 0 else near1.at[wv]
        return remote(v, v, st_send.at[D, 0], near_recv.at[D, wv], to[D])

    def own_copy(D, wv, h):
        v = z.at[mine(0), h, wv]
        return remote(v, v, own_send, ag_recv.at[D, wv, h], to[D])

    def ag_landed(D, wv, h):
        v = z.at[mine(4 - NEAR[D]), h, wv]
        return remote(v, v, own_send, ag_recv.at[D, wv, h], to[D])

    def fwd_copy(D, wv, s):
        v = z.at[mine(4 - NEAR[D]), D, wv, pl.ds(s * fr, fr)]
        dst = last.at[D] if (wv, s) == (NW - 2, FS - 1) else v
        return remote(v, dst, fwd_send, fwd_recv.at[D, wv, s], to[D])

    def d2d(v, q):
        return remote(v, v, d_send.at[q], d_recv.at[q], partner)

    def late_local(D, i):
        return pltpu.make_async_copy(z.at[chip(4 - NEAR[D]) * 2 + i, D, NW - 1], late.at[i], late_sem)

    def half_product(t, ww, j):
        return jnp.dot(xt[t].reshape(2 * rw, kd), ww[j], preferred_element_type=jnp.float32)

    def product(t, p, j):
        b = xp[p].reshape(2 * rw, kd)
        return half_product(t, w_own, j) + jnp.dot(b, w_par[j], preferred_element_type=jnp.float32)

    barrier = pltpu.get_barrier_semaphore()
    for dev in (partner, to[0], to[1]):
        pl.semaphore_signal(barrier, inc=1, device_id={"tp": dev}, device_id_type=MESH)
    x_local(3, other(2), 0).start()
    w_local(0).start()
    x_local(0, mine(2), 0).start()
    for j in range(1, NC):
        w_local(j).start()
    for wv in range(1, NW - 1):
        x_local(wv, mine(2), wv).start()
    for h in range(2):
        r_local(0, h).start()
    pltpu.make_async_copy(g, gv, g_sem).start()

    x_local(3, other(2), 0).wait()

    @pl.loop(0, NC)
    def _(j):
        w_local(j).wait()
        acc = half_product(3, w_own, j)
        for h in range(2):
            stage[h, j, 1] = acc[h * rw : (h + 1) * rw].astype(bf)

        @pl.when(j == 0)
        def _():
            pl.semaphore_wait(barrier, 3)

        pre_copy(j).start()

    for j in range(NC):
        if j == 1:
            x_remote(0, 2, 1).start()
        w_remote(j).start()
    for wv in range(2, NW):
        x_remote(0, 2, wv).start()
    for wv in range(NW):
        for D in range(2):
            x_remote(1 + D, NEAR[D], wv).start()
    for wv in range(NW):
        x_remote(3, 0, wv).start()
    x_local(3, mine(2), NW - 1).start()
    x_local(0, mine(2), 0).wait()

    @pl.loop(0, NC)
    def _(j):
        acc = half_product(0, w_own, j)
        pre_copy(j).wait_recv()
        for D in range(2):
            part = acc[D * rw : (D + 1) * rw] + pre[j, D].astype(jnp.float32)
            stage[D, j, 0] = part.astype(bf)
            far_copy(D, j, 0, j).start()

    x_local(0, mine(NEAR[0]), 0).start()
    remote(pre, pre, pre_send, pre_recv.at[0], partner).wait_send()

    @pl.loop(1, NW)
    def _(wv):
        x_local(wv, mine(2), wv).wait()
        x_landed(wv - 1, 1, wv - 1).wait_recv()

        @pl.loop(0, NC)
        def _(j):
            slot = j

            @pl.when(wv == 1)
            def _():
                w_remote(j).wait_recv()

            acc = product(wv, wv - 1, j)
            for D in range(2):
                far_copy(D, slot, wv, j).wait_send()
                stage[D, slot, 0] = acc[D * rw : (D + 1) * rw].astype(bf)
                far_copy(D, slot, wv, j).start()

        D = lax.rem(wv, 2)
        x_local(wv, mine(1 + 2 * D), lax.div(wv, 2)).start()

    x_landed(NW - 1, 2 * NW, NW - 1).wait_recv()

    @pl.loop(0, NW)
    def _(wv):
        t0 = lax.rem(2 * wv, 4)
        for D in range(2):
            x_local(t0 + D, mine(NEAR[D]), wv).wait()
            far_landed(D, wv).wait_recv()

        @pl.loop(0, NC)
        def _(j):
            slot = j
            for D in range(2):
                acc = product(t0 + D, (1 + D) * NW - 1 + wv, j)

                @pl.when(wv == 0)
                def _():
                    far_copy(D, slot, wv, j).wait_send()

                @pl.when(wv > 0)
                def _():
                    near_copy(D, slot, wv, j).wait_send()

                for h in range(2):
                    part = acc[h * rw : (h + 1) * rw]
                    if h == D:
                        part = part + far[D, wv, j].astype(jnp.float32)
                    stage[D, slot, h] = part.astype(bf)
                near_copy(D, slot, wv, j).start()

        for D in range(2):

            @pl.when(wv < 2)
            def _():
                x_local(t0 + D, mine(NEAR[D]), wv + 2).start()

            @pl.when(wv >= 2)
            def _():
                x_local(t0 + D, mine(0), 2 * (wv - 2) + D).start()

    pltpu.make_async_copy(g, gv, g_sem).wait()
    gain = gv[...].astype(jnp.float32).reshape(1, hid)
    x_landed(3 * NW - 1, NW, NW).wait_recv()

    @pl.loop(0, NW)
    def _(wv):
        x_local(wv, mine(0), wv).wait()
        for D in range(2):
            near_landed(D, wv).wait_recv()

        @pl.loop(0, NC)
        def _(j):
            acc = product(wv, 3 * NW - 1 + wv, j)
            for h in range(2):
                y = acc[h * rw : (h + 1) * rw]
                y = y + z[mine(0), h, wv, :, cols(j)].astype(jnp.float32)
                y = y + near1[wv, h, :, cols(j)].astype(jnp.float32)
                z[mine(0), h, wv, :, cols(j)] = y.astype(bf)

        for h in range(2):
            r_local(wv, h).wait()

            @pl.loop(0, rw // 16)
            def _(i):
                q = pl.ds(pl.multiple_of(i * 16, 16), 16)
                a = rt[h, q].astype(jnp.float32) + z[mine(0), h, wv, q].astype(jnp.float32)
                ms = jnp.mean(a * a, axis=-1, keepdims=True)
                z[mine(0), h, wv, q] = (a * lax.rsqrt(ms + EPS) * gain).astype(bf)

            for D in range(2):
                own_copy(D, wv, h).start()
            d2d(z.at[mine(0), h, wv], 0).start()

            @pl.when(wv < NW - 1)
            def _():
                r_local(wv + 1, h).start()

    for wv in range(NW):
        for h in range(2):
            for D in range(2):
                ag_landed(D, wv, h).wait_recv()
                if h == D and wv < NW - 1:
                    for s in range(FS):
                        fwd_copy(D, wv, s).start()
                q = 2 if wv < NW - 1 else (1 if h == D else 3)
                d2d(z.at[mine(4 - NEAR[D]), h, wv], q).start()

    def swapped(q, like):
        d2d(like, q).wait_send()
        d2d(like, q).wait_recv()

    swapped(1, z.at[0, :, 0])
    for D in range(2):

        @pl.when(k == D)
        def _():
            for i in range(2):
                late_local(D, i).start()

    @pl.loop(0, SLOTS)
    def _(slot):
        for D in range(2):
            near_copy(D, slot, 0, 0).wait_send()

    remote(xp, xp, xp_send, xp_recv.at[0], partner).wait_send()
    remote(w_par, w_par, wx_send, wx_recv.at[0], partner).wait_send()
    v = z.at[pl.ds(0, 2)]
    remote(v, v, own_send, ag_recv.at[0, 0, 0], partner).wait_send()
    swapped(0, z.at[0])
    swapped(2, z.at[pl.ds(0, 2), :, pl.ds(0, NW - 1)])
    swapped(3, z.at[0, :, 0])
    pltpu.make_async_copy(late, late, late_sem).wait()

    for wv in range(NW - 1):
        for s in range(FS):
            for D in range(2):
                fwd_copy(D, wv, s).wait_recv()
                if (wv, s) != (NW - 2, FS - 1):
                    d2d(z.at[mine(2), D, wv, pl.ds(s * fr, fr)], 4 if wv < NW - 2 else 5).start()
            if (wv, s) == (NW - 2, FS - 2):
                swapped(4, z.at[0, :, pl.ds(0, NW - 2)])
    swapped(5, z.at[0, :, 0, pl.ds(0, (FS - 1) * fr)])
    v = z.at[0, :, pl.ds(0, NW - 1)]
    remote(v, v, fwd_send, fwd_recv.at[0, 0, 0], partner).wait_send()


def store_kernel(z, o, sem):
    n = z.shape[0]
    for i in range(n):
        pltpu.make_async_copy(z.at[i], o.at[i], sem.at[i]).start()
    for i in range(n):
        pltpu.make_async_copy(z.at[i], o.at[i], sem.at[i]).wait()


def late_kernel(o_in, late, late_other, last, last_other, o, late_sem, last_sem):
    me = lax.axis_index("tp")
    k = lax.rem(me, 2)
    chip = lax.rem(lax.div(me, 2) + 2, CHIPS) * 2
    fr = last.shape[1]
    rows = pl.ds((FS - 1) * fr, fr)
    copies = []
    for n in range(2):
        v, u = (late, late_other)[n], (last, last_other)[n]
        core = k if n == 0 else 1 - k
        for i in range(2):
            dst = o.at[chip + i, core, NW - 1]
            copies.append(pltpu.make_async_copy(v.at[i], dst, late_sem.at[n, i]))
            dst = o.at[chip + core, i, NW - 2, rows]
            copies.append(pltpu.make_async_copy(u.at[i], dst, last_sem.at[n, i]))
    for copy in copies:
        copy.start()
    for copy in copies:
        copy.wait()


def solution(mesh):
    tp = mesh.shape["tp"]
    onward = [(i, (i + 2 if i % 2 == 0 else i - 2) % tp) for i in range(tp)]
    swap = [(i, i + 1 - 2 * (i % 2)) for i in range(tp)]

    def local(x, w, r, g):
        t, kd = x.shape
        hid = w.shape[1]
        half = t // tp // 2
        rw, cw = half // NW, hid // NC
        x5 = x.reshape(tp, 2, NW, rw, kd)
        r5 = r.reshape(tp, 2, NW, rw, hid)
        dma = pltpu.SemaphoreType.DMA
        bf = jnp.bfloat16
        any_spec = pl.BlockSpec(memory_space=pl.ANY)
        z, late, last = pl.pallas_call(
            ring_kernel,
            name="ring",
            out_shape=(
                pltpu.VMEM((tp, 2, NW, rw, hid), bf),
                jax.ShapeDtypeStruct((2, rw, hid), bf),
                jax.ShapeDtypeStruct((2, rw // FS, hid), bf),
            ),
            in_specs=[any_spec] * 4,
            out_specs=(pl.BlockSpec(memory_space=pltpu.VMEM), any_spec, any_spec),
            scratch_shapes=[
                pltpu.VMEM((hid,), bf),
                pltpu.VMEM((NC, kd, cw), bf),
                pltpu.VMEM((NC, kd, cw), bf),
                pltpu.VMEM((4, 2, rw, kd), bf),
                pltpu.VMEM((4 * NW - 1, 2, rw, kd), bf),
                pltpu.VMEM((NC, 2, rw, cw), bf),
                pltpu.VMEM((2, NW, NC, rw, cw), bf),
                pltpu.VMEM((NW, 2, rw, hid), bf),
                pltpu.VMEM((2, SLOTS, 2, rw, cw), bf),
                pltpu.VMEM((2, rw, hid), bf),
                dma, dma((NC,)), dma((4,)), dma((2,)), dma,
                dma, dma((NC,)), dma, dma((NW + 1,)), dma, dma((NC,)),
                dma((2, SLOTS)), dma((2, NW)), dma((2, NW)),
                dma, dma((2, NW, 2)), dma, dma((2, NW - 1, FS)), dma((6,)), dma((6,)),
            ],
            compiler_params=pltpu.CompilerParams(
                collective_id=0, has_side_effects=True, vmem_limit_bytes=33000000
            ),
        )(x5, w, r5, g)
        late = lax.ppermute(late, "tp", onward)
        last_other = lax.ppermute(last, "tp", swap)
        out = pl.pallas_call(
            store_kernel,
            name="store",
            out_shape=jax.ShapeDtypeStruct(z.shape, bf),
            in_specs=[pl.BlockSpec(memory_space=pltpu.VMEM)],
            out_specs=any_spec,
            scratch_shapes=[dma((tp,))],
            compiler_params=pltpu.CompilerParams(vmem_limit_bytes=1 << 20),
            cost_estimate=pl.CostEstimate(
                flops=10**10, bytes_accessed=2 * t * hid, transcendentals=0
            ),
        )(z)
        out, late, last_other = lax.optimization_barrier((out, late, last_other))
        out = pl.pallas_call(
            late_kernel,
            name="late",
            out_shape=jax.ShapeDtypeStruct(z.shape, bf),
            in_specs=[any_spec] * 5,
            out_specs=any_spec,
            scratch_shapes=[dma((2, 2)), dma((2, 2))],
            input_output_aliases={0: 0},
            compiler_params=pltpu.CompilerParams(vmem_limit_bytes=1 << 20),
        )(out, late, lax.ppermute(late, "tp", swap), last, last_other)
        return out.reshape(t, hid)

    return jax.shard_map(
        local,
        mesh=mesh,
        in_specs=(P("data", "tp"), P("tp", None), P("data", None), P(None)),
        out_specs=P("data", None),
        check_vma=False,
    )
```

```python
import jax
import jax.numpy as jnp
from jax import lax
from jax.experimental import pallas as pl
from jax.experimental.pallas import tpu as pltpu
from jax.sharding import PartitionSpec as P


EPS = 1e-6
MESH = pl.DeviceIdType.MESH
CHIPS = 4
NW = 4
NC = 4
FS = 2
SPLIT = 3 / 4
SLOTS = 4
NEAR = (1, 3)


def ring_kernel(
    x, w, r, g, z, late_a, late_b, last,
    gv, w_own, w_par, xt, xp, pre, far, near1, stage, rt,
    g_sem, w_sem, xt_sem, rt_sem, late_sem,
    wx_send, wx_recv, xp_send, xp_recv, pre_send, pre_recv,
    st_send, far_recv, near_recv,
    own_send, ag_recv, fwd_send, fwd_recv, d_send, d_recv,
):
    me = lax.axis_index("tp")
    k = lax.rem(me, 2)
    c = lax.div(me, 2)
    chip = lambda d: lax.rem(c + d, CHIPS)
    mine = lambda d: chip(d) * 2 + k
    other = lambda d: chip(d) * 2 + 1 - k
    partner = c * 2 + 1 - k
    to = (mine(1), mine(3))
    rw, kd = x.shape[3], x.shape[4]
    hid = w.shape[1]
    cw = hid // NC
    fr = rw // FS
    bf = jnp.bfloat16

    def remote(src, dst, ssem, rsem, dev):
        return pltpu.make_async_remote_copy(
            src_ref=src, dst_ref=dst, send_sem=ssem, recv_sem=rsem,
            device_id={"tp": dev}, device_id_type=MESH,
        )

    def cols(j):
        return pl.ds(pl.multiple_of(j * cw, cw), cw)

    def w_local(j):
        return pltpu.make_async_copy(w.at[:, cols(j)], w_own.at[j], w_sem.at[j])

    def w_remote(j):
        return remote(w.at[:, cols(j)], w_par.at[j], wx_send, wx_recv.at[j], partner)

    def x_local(t, b, wv):
        return pltpu.make_async_copy(x.at[b, :, wv], xt.at[t], xt_sem.at[t])

    def x_remote(e, d, wv):
        q = wv - 1 if e == 0 else (NW - 1 if e < 3 else NW)
        return remote(x.at[other(d), :, wv], xp.at[e * NW + wv - 1], xp_send, xp_recv.at[q], partner)

    def x_landed(first, n, q):
        v = xp.at[pl.ds(first, n)]
        return remote(v, v, xp_send, xp_recv.at[q], partner)

    def pre_copy(j):
        return remote(stage.at[:, j, 1], pre.at[j], pre_send, pre_recv.at[j], partner)

    def r_local(wv, h):
        return pltpu.make_async_copy(r.at[mine(0), h, wv], rt.at[h], rt_sem.at[h])

    def far_copy(D, slot, wv, j):
        return remote(
            stage.at[D, slot, 0], far.at[D, wv, j],
            st_send.at[D, slot], far_recv.at[D, wv], to[D],
        )

    def far_landed(D, wv):
        v = far.at[D, wv]
        return remote(v, v, st_send.at[D, 0], far_recv.at[D, wv], to[D])

    def near_copy(D, slot, wv, j):
        dst = z.at[to[0], :, wv, :, cols(j)] if D == 0 else near1.at[wv, :, :, cols(j)]
        return remote(stage.at[D, slot], dst, st_send.at[D, slot], near_recv.at[D, wv], to[D])

    def near_landed(D, wv):
        v = z.at[mine(0), :, wv] if D == 0 else near1.at[wv]
        return remote(v, v, st_send.at[D, 0], near_recv.at[D, wv], to[D])

    def own_copy(D, wv, h):
        v = z.at[mine(0), h, wv]
        return remote(v, v, own_send, ag_recv.at[D, wv, h], to[D])

    def ag_landed(D, wv, h):
        v = z.at[mine(4 - NEAR[D]), h, wv]
        return remote(v, v, own_send, ag_recv.at[D, wv, h], to[D])

    def fwd_copy(D, wv, s):
        v = z.at[mine(4 - NEAR[D]), D, wv, pl.ds(s * fr, fr)]
        dst = last.at[D] if (wv, s) == (NW - 2, FS - 1) else v
        return remote(v, dst, fwd_send, fwd_recv.at[D, wv, s], to[D])

    def d2d(v, q):
        return remote(v, v, d_send.at[q], d_recv.at[q], partner)

    def late_local(D, i):
        ra = late_a.shape[1]
        v = z.at[chip(4 - NEAR[D]) * 2 + i, D, NW - 1]
        return (
            pltpu.make_async_copy(v.at[pl.ds(0, ra)], late_a.at[i], late_sem.at[0]),
            pltpu.make_async_copy(v.at[pl.ds(ra, rw - ra)], late_b.at[i], late_sem.at[1]),
        )

    def half_product(t, ww, j):
        return jnp.dot(xt[t].reshape(2 * rw, kd), ww[j], preferred_element_type=jnp.float32)

    def product(t, p, j):
        b = xp[p].reshape(2 * rw, kd)
        return half_product(t, w_own, j) + jnp.dot(b, w_par[j], preferred_element_type=jnp.float32)

    barrier = pltpu.get_barrier_semaphore()
    for dev in (partner, to[0], to[1]):
        pl.semaphore_signal(barrier, inc=1, device_id={"tp": dev}, device_id_type=MESH)
    x_local(3, other(2), 0).start()
    w_local(0).start()
    x_local(0, mine(2), 0).start()
    for j in range(1, NC):
        w_local(j).start()
    for wv in range(1, NW - 1):
        x_local(wv, mine(2), wv).start()
    for h in range(2):
        r_local(0, h).start()
    pltpu.make_async_copy(g, gv, g_sem).start()

    x_local(3, other(2), 0).wait()

    @pl.loop(0, NC)
    def _(j):
        w_local(j).wait()
        acc = half_product(3, w_own, j)
        for h in range(2):
            stage[h, j, 1] = acc[h * rw : (h + 1) * rw].astype(bf)

        @pl.when(j == 0)
        def _():
            pl.semaphore_wait(barrier, 3)

        pre_copy(j).start()

    for j in range(NC):
        if j == 1:
            x_remote(0, 2, 1).start()
        w_remote(j).start()
    for wv in range(2, NW):
        x_remote(0, 2, wv).start()
    for wv in range(NW):
        for D in range(2):
            x_remote(1 + D, NEAR[D], wv).start()
    for wv in range(NW):
        x_remote(3, 0, wv).start()
    x_local(3, mine(2), NW - 1).start()
    x_local(0, mine(2), 0).wait()

    @pl.loop(0, NC)
    def _(j):
        acc = half_product(0, w_own, j)
        pre_copy(j).wait_recv()
        for D in range(2):
            part = acc[D * rw : (D + 1) * rw] + pre[j, D].astype(jnp.float32)
            stage[D, j, 0] = part.astype(bf)
            far_copy(D, j, 0, j).start()

    x_local(0, mine(NEAR[0]), 0).start()
    remote(pre, pre, pre_send, pre_recv.at[0], partner).wait_send()

    @pl.loop(1, NW)
    def _(wv):
        x_local(wv, mine(2), wv).wait()
        x_landed(wv - 1, 1, wv - 1).wait_recv()

        @pl.loop(0, NC)
        def _(j):
            slot = j

            @pl.when(wv == 1)
            def _():
                w_remote(j).wait_recv()

            acc = product(wv, wv - 1, j)
            for D in range(2):
                far_copy(D, slot, wv, j).wait_send()
                stage[D, slot, 0] = acc[D * rw : (D + 1) * rw].astype(bf)
                far_copy(D, slot, wv, j).start()

        D = lax.rem(wv, 2)
        x_local(wv, mine(1 + 2 * D), lax.div(wv, 2)).start()

    x_landed(NW - 1, 2 * NW, NW - 1).wait_recv()

    @pl.loop(0, NW)
    def _(wv):
        t0 = lax.rem(2 * wv, 4)
        for D in range(2):
            x_local(t0 + D, mine(NEAR[D]), wv).wait()
            far_landed(D, wv).wait_recv()

        @pl.loop(0, NC)
        def _(j):
            slot = j
            for D in range(2):
                acc = product(t0 + D, (1 + D) * NW - 1 + wv, j)

                @pl.when(wv == 0)
                def _():
                    far_copy(D, slot, wv, j).wait_send()

                @pl.when(wv > 0)
                def _():
                    near_copy(D, slot, wv, j).wait_send()

                for h in range(2):
                    part = acc[h * rw : (h + 1) * rw]
                    if h == D:
                        part = part + far[D, wv, j].astype(jnp.float32)
                    stage[D, slot, h] = part.astype(bf)
                near_copy(D, slot, wv, j).start()

        for D in range(2):

            @pl.when(wv < 2)
            def _():
                x_local(t0 + D, mine(NEAR[D]), wv + 2).start()

            @pl.when(wv >= 2)
            def _():
                x_local(t0 + D, mine(0), 2 * (wv - 2) + D).start()

    pltpu.make_async_copy(g, gv, g_sem).wait()
    gain = gv[...].astype(jnp.float32).reshape(1, hid)
    x_landed(3 * NW - 1, NW, NW).wait_recv()

    @pl.loop(0, NW)
    def _(wv):
        x_local(wv, mine(0), wv).wait()
        for D in range(2):
            near_landed(D, wv).wait_recv()

        @pl.loop(0, NC)
        def _(j):
            acc = product(wv, 3 * NW - 1 + wv, j)
            for h in range(2):
                y = acc[h * rw : (h + 1) * rw]
                y = y + z[mine(0), h, wv, :, cols(j)].astype(jnp.float32)
                y = y + near1[wv, h, :, cols(j)].astype(jnp.float32)
                z[mine(0), h, wv, :, cols(j)] = y.astype(bf)

        for h in range(2):
            r_local(wv, h).wait()

            @pl.loop(0, rw // 16)
            def _(i):
                q = pl.ds(pl.multiple_of(i * 16, 16), 16)
                a = rt[h, q].astype(jnp.float32) + z[mine(0), h, wv, q].astype(jnp.float32)
                ms = jnp.mean(a * a, axis=-1, keepdims=True)
                z[mine(0), h, wv, q] = (a * lax.rsqrt(ms + EPS) * gain).astype(bf)

            for D in range(2):
                own_copy(D, wv, h).start()
            d2d(z.at[mine(0), h, wv], 0).start()

            @pl.when(wv < NW - 1)
            def _():
                r_local(wv + 1, h).start()

    for wv in range(NW):
        for h in range(2):
            for D in range(2):
                ag_landed(D, wv, h).wait_recv()
                if h == D and wv < NW - 1:
                    for s in range(FS):
                        fwd_copy(D, wv, s).start()
                q = 2 if wv < NW - 1 else (1 if h == D else 3)
                d2d(z.at[mine(4 - NEAR[D]), h, wv], q).start()

    def swapped(q, like):
        d2d(like, q).wait_send()
        d2d(like, q).wait_recv()

    swapped(1, z.at[0, :, 0])
    for D in range(2):

        @pl.when(k == D)
        def _():
            for i in range(2):
                for copy in late_local(D, i):
                    copy.start()

    @pl.loop(0, SLOTS)
    def _(slot):
        for D in range(2):
            near_copy(D, slot, 0, 0).wait_send()

    remote(xp, xp, xp_send, xp_recv.at[0], partner).wait_send()
    remote(w_par, w_par, wx_send, wx_recv.at[0], partner).wait_send()
    v = z.at[pl.ds(0, 2)]
    remote(v, v, own_send, ag_recv.at[0, 0, 0], partner).wait_send()
    swapped(0, z.at[0])
    swapped(2, z.at[pl.ds(0, 2), :, pl.ds(0, NW - 1)])
    swapped(3, z.at[0, :, 0])
    pltpu.make_async_copy(late_a, late_a, late_sem.at[0]).wait()
    pltpu.make_async_copy(late_b, late_b, late_sem.at[1]).wait()

    for wv in range(NW - 1):
        for s in range(FS):
            for D in range(2):
                fwd_copy(D, wv, s).wait_recv()
                if (wv, s) != (NW - 2, FS - 1):
                    d2d(z.at[mine(2), D, wv, pl.ds(s * fr, fr)], 4 if wv < NW - 2 else 5).start()
            if (wv, s) == (NW - 2, FS - 2):
                swapped(4, z.at[0, :, pl.ds(0, NW - 2)])
    swapped(5, z.at[0, :, 0, pl.ds(0, (FS - 1) * fr)])
    v = z.at[0, :, pl.ds(0, NW - 1)]
    remote(v, v, fwd_send, fwd_recv.at[0, 0, 0], partner).wait_send()


def store_kernel(z, o, sem):
    n = z.shape[0]
    for i in range(n):
        pltpu.make_async_copy(z.at[i], o.at[i], sem.at[i]).start()
    for i in range(n):
        pltpu.make_async_copy(z.at[i], o.at[i], sem.at[i]).wait()


def place(copies):
    for copy in copies:
        copy.start()
    for copy in copies:
        copy.wait()


def across():
    me = lax.axis_index("tp")
    return lax.rem(me, 2), lax.rem(lax.div(me, 2) + 2, CHIPS) * 2


def middle_kernel(o_in, late_a, last, last_other, o, sem):
    k, chip = across()
    ra, fr = late_a.shape[1], last.shape[1]
    rows = pl.ds((FS - 1) * fr, fr)
    copies = []
    for i in range(2):
        for n, (src, dst) in enumerate((
            (late_a.at[i], o.at[chip + i, k, NW - 1, pl.ds(0, ra)]),
            (last.at[i], o.at[chip + k, i, NW - 2, rows]),
            (last_other.at[i], o.at[chip + 1 - k, i, NW - 2, rows]),
        )):
            copies.append(pltpu.make_async_copy(src, dst, sem.at[n, i]))
    place(copies)


def late_kernel(o_in, late_b, late_a_other, late_b_other, o, sem):
    k, chip = across()
    ra, rb = late_a_other.shape[1], late_b.shape[1]
    copies = []
    for i in range(2):
        for n, (src, half, rows) in enumerate((
            (late_b, k, pl.ds(ra, rb)),
            (late_a_other, 1 - k, pl.ds(0, ra)),
            (late_b_other, 1 - k, pl.ds(ra, rb)),
        )):
            dst = o.at[chip + i, half, NW - 1, rows]
            copies.append(pltpu.make_async_copy(src.at[i], dst, sem.at[n, i]))
    place(copies)


def solution(mesh):
    tp = mesh.shape["tp"]
    onward = [(i, (i + 2 if i % 2 == 0 else i - 2) % tp) for i in range(tp)]
    swap = [(i, i + 1 - 2 * (i % 2)) for i in range(tp)]

    def body(x, w, r, g):
        t, kd = x.shape
        hid = w.shape[1]
        half = t // tp // 2
        rw, cw = half // NW, hid // NC
        ra = int(rw * SPLIT)
        x5 = x.reshape(tp, 2, NW, rw, kd)
        r5 = r.reshape(tp, 2, NW, rw, hid)
        dma = pltpu.SemaphoreType.DMA
        bf = jnp.bfloat16
        any_spec = pl.BlockSpec(memory_space=pl.ANY)
        z, late_a, late_b, last = pl.pallas_call(
            ring_kernel,
            name="ring",
            out_shape=(
                pltpu.VMEM((tp, 2, NW, rw, hid), bf),
                jax.ShapeDtypeStruct((2, ra, hid), bf),
                jax.ShapeDtypeStruct((2, rw - ra, hid), bf),
                jax.ShapeDtypeStruct((2, rw // FS, hid), bf),
            ),
            in_specs=[any_spec] * 4,
            out_specs=(pl.BlockSpec(memory_space=pltpu.VMEM), any_spec, any_spec, any_spec),
            scratch_shapes=[
                pltpu.VMEM((hid,), bf),
                pltpu.VMEM((NC, kd, cw), bf),
                pltpu.VMEM((NC, kd, cw), bf),
                pltpu.VMEM((4, 2, rw, kd), bf),
                pltpu.VMEM((4 * NW - 1, 2, rw, kd), bf),
                pltpu.VMEM((NC, 2, rw, cw), bf),
                pltpu.VMEM((2, NW, NC, rw, cw), bf),
                pltpu.VMEM((NW, 2, rw, hid), bf),
                pltpu.VMEM((2, SLOTS, 2, rw, cw), bf),
                pltpu.VMEM((2, rw, hid), bf),
                dma, dma((NC,)), dma((4,)), dma((2,)), dma((2,)),
                dma, dma((NC,)), dma, dma((NW + 1,)), dma, dma((NC,)),
                dma((2, SLOTS)), dma((2, NW)), dma((2, NW)),
                dma, dma((2, NW, 2)), dma, dma((2, NW - 1, FS)), dma((6,)), dma((6,)),
            ],
            compiler_params=pltpu.CompilerParams(
                collective_id=0, has_side_effects=True, vmem_limit_bytes=33000000
            ),
        )(x5, w, r5, g)
        late_a = lax.ppermute(late_a, "tp", onward)
        late_b = lax.ppermute(late_b, "tp", onward)
        last_other = lax.ppermute(last, "tp", swap)
        out = pl.pallas_call(
            store_kernel,
            name="store",
            out_shape=jax.ShapeDtypeStruct(z.shape, bf),
            in_specs=[pl.BlockSpec(memory_space=pltpu.VMEM)],
            out_specs=any_spec,
            scratch_shapes=[dma((tp,))],
            compiler_params=pltpu.CompilerParams(vmem_limit_bytes=1 << 20),
            cost_estimate=pl.CostEstimate(
                flops=10**10, bytes_accessed=2 * t * hid, transcendentals=0
            ),
        )(z)
        out, late_a, last_other = lax.optimization_barrier((out, late_a, last_other))
        late_a_other = lax.ppermute(late_a, "tp", swap)

        def in_place(kernel, *args):
            return pl.pallas_call(
                kernel,
                out_shape=jax.ShapeDtypeStruct(z.shape, bf),
                in_specs=[any_spec] * len(args),
                out_specs=any_spec,
                scratch_shapes=[dma((3, 2))],
                input_output_aliases={0: 0},
                compiler_params=pltpu.CompilerParams(vmem_limit_bytes=1 << 20),
                cost_estimate=pl.CostEstimate(
                    flops=10**9, bytes_accessed=t * hid // 4, transcendentals=0
                ),
            )(*args)

        out = in_place(middle_kernel, out, late_a, last, last_other)
        out, late_b = lax.optimization_barrier((out, late_b))
        late_b_other = lax.ppermute(late_b, "tp", swap)
        out = in_place(late_kernel, out, late_b, late_a_other, late_b_other)
        return out.reshape(t, hid)

    return jax.shard_map(
        body,
        mesh=mesh,
        in_specs=(P("data", "tp"), P("tp", None), P("data", None), P(None)),
        out_specs=P("data", None),
        check_vma=False,
    )
```

```python
import jax
import jax.numpy as jnp
from jax import lax
from jax.experimental import pallas as pl
from jax.experimental.pallas import tpu as pltpu
from jax.sharding import PartitionSpec as P


EPS = 1e-6
MESH = pl.DeviceIdType.MESH
CHIPS = 4
NW = 4
NC = 4
R0, R1, R2, R3 = 192, 288, 368, 480
STEP = 64
SLOTS = 4
FIRST = 128
NEAR = (1, 3)


def ring_kernel(
    x, w, r, g, z, late_a1, late_a2, late_b, last,
    gv, w_own, w_par, xt, xp, pre, far, near1, stage, rt,
    g_sem, w_sem, xt_sem, rt_sem, late_sem,
    wx_send, wx_recv, xp_send, xp_recv, pre_send, pre_recv,
    st_send, far_recv, near_recv,
    own_send, ag_recv, fwd_send, fwd_recv, last_send, last_recv, d_send, d_recv,
):
    me = lax.axis_index("tp")
    k = lax.rem(me, 2)
    c = lax.div(me, 2)
    chip = lambda d: lax.rem(c + d, CHIPS)
    mine = lambda d: chip(d) * 2 + k
    other = lambda d: chip(d) * 2 + 1 - k
    partner = c * 2 + 1 - k
    to = (mine(1), mine(3))
    rw, kd = x.shape[3], x.shape[4]
    half = NW * rw
    ranges = [(lo, min(lo + STEP, R0)) for lo in range(0, R0, STEP)]
    hid = w.shape[1]
    cw = hid // NC
    bf = jnp.bfloat16

    def remote(src, dst, ssem, rsem, dev):
        return pltpu.make_async_remote_copy(
            src_ref=src, dst_ref=dst, send_sem=ssem, recv_sem=rsem,
            device_id={"tp": dev}, device_id_type=MESH,
        )

    def cols(j):
        return pl.ds(pl.multiple_of(j * cw, cw), cw)

    def wave(wv):
        return pl.ds(pl.multiple_of(wv * rw, rw), rw)

    def w_local(j):
        return pltpu.make_async_copy(w.at[:, cols(j)], w_own.at[j], w_sem.at[j])

    def w_local_part(lo, hi, q):
        v = pl.ds(lo, hi - lo)
        return pltpu.make_async_copy(w.at[:, v], w_own.at[0, :, v], w_sem.at[q])

    def w_remote(j):
        return remote(w.at[:, cols(j)], w_par.at[j], wx_send, wx_recv, partner)

    def x_local(t, b, wv):
        return pltpu.make_async_copy(x.at[b, :, wv], xt.at[t], xt_sem.at[t])

    def x_remote(e, d, wv):
        q = wv - 1 if e == 0 else (NW - 1 if e < 3 else NW)
        return remote(x.at[other(d), :, wv], xp.at[e * NW + wv - 1], xp_send, xp_recv.at[q], partner)

    def x_landed(first, n, q):
        v = xp.at[pl.ds(first, n)]
        return remote(v, v, xp_send, xp_recv.at[q], partner)

    def pre_copy(j):
        return remote(stage.at[:, j, 1], pre.at[j], pre_send, pre_recv.at[j], partner)

    def pre_part(lo, hi, q):
        v = pl.ds(lo, hi - lo)
        return remote(stage.at[:, 0, 1, :, v], pre.at[0, :, :, v], pre_send, pre_recv.at[q], partner)

    def r_local(wv, h):
        return pltpu.make_async_copy(r.at[mine(0), h, wv], rt.at[h], rt_sem.at[h])

    def far_copy(D, slot, wv, j):
        return remote(
            stage.at[D, slot, 0], far.at[D, wv, j],
            st_send.at[D, slot], far_recv.at[D, wv], to[D],
        )

    def far_part(D, lo, hi):
        v = pl.ds(lo, hi - lo)
        sems = st_send.at[D, 0], far_recv.at[D, 0]
        return remote(stage.at[D, 0, 0, :, v], far.at[D, 0, 0, :, v], *sems, to[D])

    def far_landed(D, wv):
        v = far.at[D, wv]
        return remote(v, v, st_send.at[D, 0], far_recv.at[D, wv], to[D])

    def near_copy(D, slot, wv, j):
        dst = z.at[to[0], :, wave(wv), cols(j)] if D == 0 else near1.at[wv, :, :, cols(j)]
        return remote(stage.at[D, slot], dst, st_send.at[D, slot], near_recv.at[D, wv], to[D])

    def near_landed(D, wv):
        v = z.at[mine(0), :, wave(wv)] if D == 0 else near1.at[wv]
        return remote(v, v, st_send.at[D, 0], near_recv.at[D, wv], to[D])

    def own_copy(D, wv, h):
        v = z.at[mine(0), h, wave(wv)]
        return remote(v, v, own_send, ag_recv.at[D, wv, h], to[D])

    def ag_landed(D, wv, h):
        v = z.at[mine(4 - NEAR[D]), h, wave(wv)]
        return remote(v, v, own_send, ag_recv.at[D, wv, h], to[D])

    def fwd_copy(D, n):
        lo, hi = ranges[n]
        v = z.at[mine(4 - NEAR[D]), D, pl.ds(lo, hi - lo)]
        return remote(v, v, fwd_send, fwd_recv.at[D, n], to[D])

    def last_copy(D, i):
        v = z.at[chip(4 - NEAR[D]) * 2 + i, D, pl.ds(R0, R1 - R0)]
        return remote(v, last.at[i, D], last_send, last_recv, to[D])

    def d2d(v, q):
        return remote(v, v, d_send.at[q], d_recv.at[q], partner)

    def late_local(D, i):
        src = lambda D, lo, hi: z.at[chip(4 - NEAR[D]) * 2 + i, D, pl.ds(lo, hi - lo)]
        return (
            pltpu.make_async_copy(src(D, R2, R3), late_a1.at[i], late_sem.at[0]),
            pltpu.make_async_copy(src(D, R3, half), late_a2.at[i], late_sem.at[1]),
            pltpu.make_async_copy(src(1 - D, R1, R2), late_b.at[i], late_sem.at[2]),
        )

    def half_product(t, ww, j):
        return jnp.dot(xt[t].reshape(2 * rw, kd), ww[j], preferred_element_type=jnp.float32)

    def part_product(t, lo, hi):
        a = xt[t].reshape(2 * rw, kd)
        return jnp.dot(a, w_own[0, :, lo:hi], preferred_element_type=jnp.float32)

    def product(t, p, j):
        b = xp[p].reshape(2 * rw, kd)
        return half_product(t, w_own, j) + jnp.dot(b, w_par[j], preferred_element_type=jnp.float32)

    parts = (0, FIRST, 0), (FIRST, cw, NC)
    barrier = pltpu.get_barrier_semaphore()
    for dev in (partner, to[0], to[1]):
        pl.semaphore_signal(barrier, inc=1, device_id={"tp": dev}, device_id_type=MESH)
    x_local(3, other(2), 0).start()
    for part in parts:
        w_local_part(*part).start()
    x_local(0, mine(2), 0).start()
    for j in range(1, NC):
        w_local(j).start()
    for wv in range(1, NW - 1):
        x_local(wv, mine(2), wv).start()
    for h in range(2):
        r_local(0, h).start()
    pltpu.make_async_copy(g, gv, g_sem).start()

    x_local(3, other(2), 0).wait()

    for lo, hi, q in parts:
        w_local_part(lo, hi, q).wait()
        acc = part_product(3, lo, hi)
        for h in range(2):
            stage[h, 0, 1, :, lo:hi] = acc[h * rw : (h + 1) * rw].astype(bf)
        if lo == 0:
            pl.semaphore_wait(barrier, 3)
        pre_part(lo, hi, q).start()

    @pl.loop(1, NC)
    def _(j):
        w_local(j).wait()
        acc = half_product(3, w_own, j)
        for h in range(2):
            stage[h, j, 1] = acc[h * rw : (h + 1) * rw].astype(bf)
        pre_copy(j).start()

    x_local(3, mine(2), NW - 1).start()
    x_local(0, mine(2), 0).wait()

    for lo, hi, q in parts:
        acc = part_product(0, lo, hi)
        pre_part(lo, hi, q).wait_recv()
        for D in range(2):
            part = acc[D * rw : (D + 1) * rw] + pre[0, D, :, lo:hi].astype(jnp.float32)
            stage[D, 0, 0, :, lo:hi] = part.astype(bf)
            far_part(D, lo, hi).start()

    for j in range(NC):
        if j == 1:
            x_remote(0, 2, 1).start()
        w_remote(j).start()
    for wv in range(2, NW):
        x_remote(0, 2, wv).start()
    for wv in range(NW):
        for D in range(2):
            x_remote(1 + D, NEAR[D], wv).start()
    for wv in range(NW):
        x_remote(3, 0, wv).start()

    @pl.loop(1, NC)
    def _(j):
        acc = half_product(0, w_own, j)
        pre_copy(j).wait_recv()
        for D in range(2):
            part = acc[D * rw : (D + 1) * rw] + pre[j, D].astype(jnp.float32)
            stage[D, j, 0] = part.astype(bf)
            far_copy(D, j, 0, j).start()

    x_local(0, mine(NEAR[0]), 0).start()
    remote(pre, pre, pre_send, pre_recv.at[0], partner).wait_send()

    @pl.loop(1, NW)
    def _(wv):
        x_local(wv, mine(2), wv).wait()
        x_landed(wv - 1, 1, wv - 1).wait_recv()

        @pl.when(wv == 1)
        def _():
            remote(w_par, w_par, wx_send, wx_recv, partner).wait_recv()

        @pl.loop(0, NC)
        def _(j):
            slot = j

            acc = product(wv, wv - 1, j)
            for D in range(2):
                far_copy(D, slot, wv, j).wait_send()
                stage[D, slot, 0] = acc[D * rw : (D + 1) * rw].astype(bf)
                far_copy(D, slot, wv, j).start()

        D = lax.rem(wv, 2)
        x_local(wv, mine(1 + 2 * D), lax.div(wv, 2)).start()

    x_landed(NW - 1, 2 * NW, NW - 1).wait_recv()

    @pl.loop(0, NW)
    def _(wv):
        t0 = lax.rem(2 * wv, 4)
        for D in range(2):
            x_local(t0 + D, mine(NEAR[D]), wv).wait()
            far_landed(D, wv).wait_recv()

        @pl.loop(0, NC)
        def _(j):
            slot = j
            for D in range(2):
                acc = product(t0 + D, (1 + D) * NW - 1 + wv, j)

                @pl.when(wv == 0)
                def _():
                    far_copy(D, slot, wv, j).wait_send()

                @pl.when(wv > 0)
                def _():
                    near_copy(D, slot, wv, j).wait_send()

                for h in range(2):
                    part = acc[h * rw : (h + 1) * rw]
                    if h == D:
                        part = part + far[D, wv, j].astype(jnp.float32)
                    stage[D, slot, h] = part.astype(bf)
                near_copy(D, slot, wv, j).start()

        for D in range(2):

            @pl.when(wv < 2)
            def _():
                x_local(t0 + D, mine(NEAR[D]), wv + 2).start()

            @pl.when(wv >= 2)
            def _():
                x_local(t0 + D, mine(0), 2 * (wv - 2) + D).start()

    pltpu.make_async_copy(g, gv, g_sem).wait()
    gain = gv[...].astype(jnp.float32).reshape(1, hid)
    x_landed(3 * NW - 1, NW, NW).wait_recv()

    @pl.loop(0, NW)
    def _(wv):
        x_local(wv, mine(0), wv).wait()
        for D in range(2):
            near_landed(D, wv).wait_recv()

        @pl.loop(0, NC)
        def _(j):
            acc = product(wv, 3 * NW - 1 + wv, j)
            for h in range(2):
                y = acc[h * rw : (h + 1) * rw]
                y = y + z[mine(0), h, wave(wv), cols(j)].astype(jnp.float32)
                y = y + near1[wv, h, :, cols(j)].astype(jnp.float32)
                z[mine(0), h, wave(wv), cols(j)] = y.astype(bf)

        for h in range(2):
            r_local(wv, h).wait()

            @pl.loop(0, rw // 16)
            def _(i):
                q = pl.ds(pl.multiple_of(i * 16, 16), 16)
                p = pl.ds(pl.multiple_of(wv * rw + i * 16, 16), 16)
                a = rt[h, q].astype(jnp.float32) + z[mine(0), h, p].astype(jnp.float32)
                ms = jnp.mean(a * a, axis=-1, keepdims=True)
                z[mine(0), h, p] = (a * lax.rsqrt(ms + EPS) * gain).astype(bf)

            for D in range(2):
                own_copy(D, wv, h).start()
            d2d(z.at[mine(0), h, wave(wv)], 0).start()

            @pl.when(wv < NW - 1)
            def _():
                r_local(wv + 1, h).start()

    for wv in range(NW):
        for h in range(2):
            for D in range(2):
                ag_landed(D, wv, h).wait_recv()
                for n, (lo, hi) in enumerate(ranges):
                    if h == D and lo // rw == wv:
                        fwd_copy(D, n).start()
                d2d(z.at[mine(4 - NEAR[D]), h, wave(wv)], 1).start()

    def swapped(q, like):
        d2d(like, q).wait_send()
        d2d(like, q).wait_recv()

    swapped(1, z.at[pl.ds(0, 2)])

    @pl.when(k == 1)
    def _():
        for D in range(2):
            for i in range(2):
                last_copy(D, i).start()

    for D in range(2):

        @pl.when(k == D)
        def _():
            for i in range(2):
                for copy in late_local(D, i):
                    copy.start()

    @pl.loop(0, SLOTS)
    def _(slot):
        for D in range(2):
            near_copy(D, slot, 0, 0).wait_send()

    remote(xp, xp, xp_send, xp_recv.at[0], partner).wait_send()
    remote(w_par, w_par, wx_send, wx_recv, partner).wait_send()
    v = z.at[pl.ds(0, 2)]
    remote(v, v, own_send, ag_recv.at[0, 0, 0], partner).wait_send()
    swapped(0, z.at[0])
    for n, v in enumerate((late_a1, late_a2, late_b)):
        pltpu.make_async_copy(v, v, late_sem.at[n]).wait()

    for n, (lo, hi) in enumerate(ranges):
        for D in range(2):
            fwd_copy(D, n).wait_recv()
            d2d(z.at[mine(2), D, pl.ds(lo, hi - lo)], 2).start()
    v = z.at[0, :, pl.ds(0, R0)]
    remote(v, v, fwd_send, fwd_recv.at[0, 0], partner).wait_send()
    swapped(2, v)

    @pl.when(k == 1)
    def _():
        remote(last, last, last_send, last_recv, to[0]).wait()


def store_kernel(z, o, sem):
    n = z.shape[0]
    for i in range(n):
        pltpu.make_async_copy(z.at[i], o.at[i], sem.at[i]).start()
    for i in range(n):
        pltpu.make_async_copy(z.at[i], o.at[i], sem.at[i]).wait()


def place(copies):
    for copy in copies:
        copy.start()
    for copy in copies:
        copy.wait()


def across():
    me = lax.axis_index("tp")
    return lax.rem(me, 2), lax.rem(lax.div(me, 2) + 2, CHIPS) * 2


def rows_of(o, b, h, lo, hi):
    return o.at[b, h, pl.ds(lo, hi - lo)]


def last_kernel(o_in, late_b, last, last_other, o, sem):
    k, chip = across()
    rest = [(late_b.at[i], rows_of(o, chip + i, 1 - k, R1, R2)) for i in range(2)]
    for core, v in enumerate((last_other, last)):

        @pl.when(k == core)
        def _():
            pairs = rest + [
                (v.at[i, D], rows_of(o, chip + i, D, R0, R1)) for i in range(2) for D in range(2)
            ]
            place([pltpu.make_async_copy(*p, sem.at[n]) for n, p in enumerate(pairs)])


def middle_kernel(o_in, late_a1, late_b_other, o, sem):
    k, chip = across()
    pairs = []
    for i in range(2):
        pairs.append((late_a1.at[i], rows_of(o, chip + i, k, R2, R3)))
        pairs.append((late_b_other.at[i], rows_of(o, chip + i, k, R1, R2)))
    place([pltpu.make_async_copy(*p, sem.at[n]) for n, p in enumerate(pairs)])


def late_kernel(o_in, late_a2, late_a1_other, late_a2_other, o, sem):
    k, chip = across()
    half = o.shape[2]
    pairs = []
    for i in range(2):
        pairs.append((late_a2.at[i], rows_of(o, chip + i, k, R3, half)))
        pairs.append((late_a1_other.at[i], rows_of(o, chip + i, 1 - k, R2, R3)))
        pairs.append((late_a2_other.at[i], rows_of(o, chip + i, 1 - k, R3, half)))
    place([pltpu.make_async_copy(*p, sem.at[n]) for n, p in enumerate(pairs)])


def solution(mesh):
    tp = mesh.shape["tp"]
    onward = [(i, (i + 2 if i % 2 == 0 else i - 2) % tp) for i in range(tp)]
    back = [(i, (i - 2 if i % 2 == 0 else i + 2) % tp) for i in range(tp)]
    down = [(i + 1, i) for i in range(0, tp, 2)]
    swap = [(i, i + 1 - 2 * (i % 2)) for i in range(tp)]

    def body(x, w, r, g):
        t, kd = x.shape
        hid = w.shape[1]
        half = t // tp // 2
        rw, cw = half // NW, hid // NC
        x5 = x.reshape(tp, 2, NW, rw, kd)
        r5 = r.reshape(tp, 2, NW, rw, hid)
        dma = pltpu.SemaphoreType.DMA
        bf = jnp.bfloat16
        any_spec = pl.BlockSpec(memory_space=pl.ANY)
        z, late_a1, late_a2, late_b, last = pl.pallas_call(
            ring_kernel,
            name="ring",
            out_shape=(
                pltpu.VMEM((tp, 2, half, hid), bf),
                jax.ShapeDtypeStruct((2, R3 - R2, hid), bf),
                jax.ShapeDtypeStruct((2, half - R3, hid), bf),
                jax.ShapeDtypeStruct((2, R2 - R1, hid), bf),
                jax.ShapeDtypeStruct((2, 2, R1 - R0, hid), bf),
            ),
            in_specs=[any_spec] * 4,
            out_specs=(pl.BlockSpec(memory_space=pltpu.VMEM),) + (any_spec,) * 4,
            scratch_shapes=[
                pltpu.VMEM((hid,), bf),
                pltpu.VMEM((NC, kd, cw), bf),
                pltpu.VMEM((NC, kd, cw), bf),
                pltpu.VMEM((4, 2, rw, kd), bf),
                pltpu.VMEM((4 * NW - 1, 2, rw, kd), bf),
                pltpu.VMEM((NC, 2, rw, cw), bf),
                pltpu.VMEM((2, NW, NC, rw, cw), bf),
                pltpu.VMEM((NW, 2, rw, hid), bf),
                pltpu.VMEM((2, SLOTS, 2, rw, cw), bf),
                pltpu.VMEM((2, rw, hid), bf),
                dma, dma((NC + 1,)), dma((4,)), dma((2,)), dma((3,)),
                dma, dma, dma, dma((NW + 1,)), dma, dma((NC + 1,)),
                dma((2, SLOTS)), dma((2, NW)), dma((2, NW)),
                dma, dma((2, NW, 2)), dma, dma((2, -(-R0 // STEP))), dma, dma, dma((3,)), dma((3,)),
            ],
            compiler_params=pltpu.CompilerParams(
                collective_id=0, has_side_effects=True, vmem_limit_bytes=33000000
            ),
        )(x5, w, r5, g)
        late_a1 = lax.ppermute(late_a1, "tp", onward)
        late_b = lax.ppermute(late_b, "tp", back)
        late_a2 = lax.ppermute(late_a2, "tp", onward)
        last_other = lax.ppermute(last, "tp", down)
        out = pl.pallas_call(
            store_kernel,
            name="store",
            out_shape=jax.ShapeDtypeStruct(z.shape, bf),
            in_specs=[pl.BlockSpec(memory_space=pltpu.VMEM)],
            out_specs=any_spec,
            scratch_shapes=[dma((tp,))],
            compiler_params=pltpu.CompilerParams(vmem_limit_bytes=1 << 20),
            cost_estimate=pl.CostEstimate(
                flops=10**10, bytes_accessed=2 * t * hid, transcendentals=0
            ),
        )(z)
        out, late_b, last_other = lax.optimization_barrier((out, late_b, last_other))
        late_b_other = lax.ppermute(late_b, "tp", swap)

        def in_place(kernel, *args):
            return pl.pallas_call(
                kernel,
                out_shape=jax.ShapeDtypeStruct(z.shape, bf),
                in_specs=[any_spec] * len(args),
                out_specs=any_spec,
                scratch_shapes=[dma((6,))],
                input_output_aliases={0: 0},
                compiler_params=pltpu.CompilerParams(vmem_limit_bytes=1 << 20),
                cost_estimate=pl.CostEstimate(
                    flops=10**9, bytes_accessed=t * hid // 4, transcendentals=0
                ),
            )(*args)

        out = in_place(last_kernel, out, late_b, last, last_other)
        out, late_a1 = lax.optimization_barrier((out, late_a1))
        late_a1_other = lax.ppermute(late_a1, "tp", swap)
        out = in_place(middle_kernel, out, late_a1, late_b_other)
        out, late_a2 = lax.optimization_barrier((out, late_a2))
        late_a2_other = lax.ppermute(late_a2, "tp", swap)
        out = in_place(late_kernel, out, late_a2, late_a1_other, late_a2_other)
        return out.reshape(t, hid)

    return jax.shard_map(
        body,
        mesh=mesh,
        in_specs=(P("data", "tp"), P("tp", None), P("data", None), P(None)),
        out_specs=P("data", None),
        check_vma=False,
    )
```

```python
import jax
import jax.numpy as jnp
from jax import lax
from jax.experimental import pallas as pl
from jax.experimental.pallas import tpu as pltpu
from jax.sharding import PartitionSpec as P


EPS = 1e-6
MESH = pl.DeviceIdType.MESH
CHIPS = 4
NW = 4
NC = 4
R0, R1, R2, R3 = 192, 288, 368, 496
STEP = 64
SLOTS = 4
FIRST = 128
NEAR = (1, 3)


def ring_kernel(
    x, w, r, g, z, late_a1, late_a2, late_b, last,
    gv, w_own, w_par, xt, xp, pre, far, near1, stage, rt,
    g_sem, w_sem, xt_sem, rt_sem, late_sem,
    wx_send, wx_recv, xp_send, xp_recv, pre_send, pre_recv,
    st_send, far_recv, near_recv,
    own_send, ag_recv, fwd_send, fwd_recv, last_send, last_recv, d_send, d_recv,
):
    me = lax.axis_index("tp")
    k = lax.rem(me, 2)
    c = lax.div(me, 2)
    chip = lambda d: lax.rem(c + d, CHIPS)
    mine = lambda d: chip(d) * 2 + k
    other = lambda d: chip(d) * 2 + 1 - k
    partner = c * 2 + 1 - k
    to = (mine(1), mine(3))
    rw, kd = x.shape[3], x.shape[4]
    half = NW * rw
    ranges = [(lo, min(lo + STEP, R0)) for lo in range(0, R0, STEP)]
    hid = w.shape[1]
    cw = hid // NC
    bf = jnp.bfloat16

    def remote(src, dst, ssem, rsem, dev):
        return pltpu.make_async_remote_copy(
            src_ref=src, dst_ref=dst, send_sem=ssem, recv_sem=rsem,
            device_id={"tp": dev}, device_id_type=MESH,
        )

    def cols(j):
        return pl.ds(pl.multiple_of(j * cw, cw), cw)

    def wave(wv):
        return pl.ds(pl.multiple_of(wv * rw, rw), rw)

    def w_local(j):
        return pltpu.make_async_copy(w.at[:, cols(j)], w_own.at[j], w_sem.at[j])

    def w_local_part(lo, hi, q):
        v = pl.ds(lo, hi - lo)
        return pltpu.make_async_copy(w.at[:, v], w_own.at[0, :, v], w_sem.at[q])

    def w_remote(j):
        return remote(w.at[:, cols(j)], w_par.at[j], wx_send, wx_recv, partner)

    def x_local(t, b, wv):
        return pltpu.make_async_copy(x.at[b, :, wv], xt.at[t], xt_sem.at[t])

    def x_remote(e, d, wv):
        q = wv - 1 if e == 0 else (NW - 1 if e < 3 else NW)
        return remote(x.at[other(d), :, wv], xp.at[e * NW + wv - 1], xp_send, xp_recv.at[q], partner)

    def x_landed(first, n, q):
        v = xp.at[pl.ds(first, n)]
        return remote(v, v, xp_send, xp_recv.at[q], partner)

    def pre_copy(j):
        return remote(stage.at[:, j, 1], pre.at[j], pre_send, pre_recv.at[j], partner)

    def pre_part(lo, hi, q):
        v = pl.ds(lo, hi - lo)
        return remote(stage.at[:, 0, 1, :, v], pre.at[0, :, :, v], pre_send, pre_recv.at[q], partner)

    def r_local(wv, h):
        return pltpu.make_async_copy(r.at[mine(0), h, wv], rt.at[h], rt_sem.at[h])

    def far_copy(D, slot, wv, j):
        return remote(
            stage.at[D, slot, 0], far.at[D, wv, j],
            st_send.at[D, slot], far_recv.at[D, wv], to[D],
        )

    def far_part(D, lo, hi):
        v = pl.ds(lo, hi - lo)
        sems = st_send.at[D, 0], far_recv.at[D, 0]
        return remote(stage.at[D, 0, 0, :, v], far.at[D, 0, 0, :, v], *sems, to[D])

    def far_landed(D, wv):
        v = far.at[D, wv]
        return remote(v, v, st_send.at[D, 0], far_recv.at[D, wv], to[D])

    def near_copy(D, slot, wv, j):
        dst = z.at[to[0], :, wave(wv), cols(j)] if D == 0 else near1.at[wv, :, :, cols(j)]
        return remote(stage.at[D, slot], dst, st_send.at[D, slot], near_recv.at[D, wv], to[D])

    def near_landed(D, wv):
        v = z.at[mine(0), :, wave(wv)] if D == 0 else near1.at[wv]
        return remote(v, v, st_send.at[D, 0], near_recv.at[D, wv], to[D])

    def own_copy(D, wv, h):
        v = z.at[mine(0), h, wave(wv)]
        return remote(v, v, own_send, ag_recv.at[D, wv, h], to[D])

    def ag_landed(D, wv, h):
        v = z.at[mine(4 - NEAR[D]), h, wave(wv)]
        return remote(v, v, own_send, ag_recv.at[D, wv, h], to[D])

    def fwd_copy(D, n):
        lo, hi = ranges[n]
        v = z.at[mine(4 - NEAR[D]), D, pl.ds(lo, hi - lo)]
        return remote(v, v, fwd_send, fwd_recv.at[D, n], to[D])

    def last_copy(D, i):
        v = z.at[chip(4 - NEAR[D]) * 2 + i, D, pl.ds(R0, R1 - R0)]
        return remote(v, last.at[i, D], last_send, last_recv, to[D])

    def d2d(v, q):
        return remote(v, v, d_send.at[q], d_recv.at[q], partner)

    def late_local(D, i):
        src = lambda D, lo, hi: z.at[chip(4 - NEAR[D]) * 2 + i, D, pl.ds(lo, hi - lo)]
        return (
            pltpu.make_async_copy(src(D, R2, R3), late_a1.at[i], late_sem.at[0]),
            pltpu.make_async_copy(src(D, R3, half), late_a2.at[i], late_sem.at[1]),
            pltpu.make_async_copy(src(1 - D, R1, R2), late_b.at[i], late_sem.at[2]),
        )

    def half_product(t, ww, j):
        return jnp.dot(xt[t].reshape(2 * rw, kd), ww[j], preferred_element_type=jnp.float32)

    def part_product(t, lo, hi):
        a = xt[t].reshape(2 * rw, kd)
        return jnp.dot(a, w_own[0, :, lo:hi], preferred_element_type=jnp.float32)

    def product(t, p, j):
        b = xp[p].reshape(2 * rw, kd)
        return half_product(t, w_own, j) + jnp.dot(b, w_par[j], preferred_element_type=jnp.float32)

    parts = (0, FIRST, 0), (FIRST, cw, NC)
    barrier = pltpu.get_barrier_semaphore()
    for dev in (partner, to[0], to[1]):
        pl.semaphore_signal(barrier, inc=1, device_id={"tp": dev}, device_id_type=MESH)
    x_local(3, other(2), 0).start()
    for part in parts:
        w_local_part(*part).start()
    x_local(0, mine(2), 0).start()
    for j in range(1, NC):
        w_local(j).start()
    for wv in range(1, NW - 1):
        x_local(wv, mine(2), wv).start()
    for h in range(2):
        r_local(0, h).start()
    pltpu.make_async_copy(g, gv, g_sem).start()

    x_local(3, other(2), 0).wait()

    for lo, hi, q in parts:
        w_local_part(lo, hi, q).wait()
        acc = part_product(3, lo, hi)
        for h in range(2):
            stage[h, 0, 1, :, lo:hi] = acc[h * rw : (h + 1) * rw].astype(bf)
        if lo == 0:
            pl.semaphore_wait(barrier, 3)
        pre_part(lo, hi, q).start()

    x_local(0, mine(2), 0).wait()

    for lo, hi, q in parts:
        acc = part_product(0, lo, hi)
        pre_part(lo, hi, q).wait_recv()
        for D in range(2):
            part = acc[D * rw : (D + 1) * rw] + pre[0, D, :, lo:hi].astype(jnp.float32)
            stage[D, 0, 0, :, lo:hi] = part.astype(bf)
            far_part(D, lo, hi).start()

    @pl.loop(1, NC)
    def _(j):
        w_local(j).wait()
        acc = half_product(3, w_own, j)
        for h in range(2):
            stage[h, j, 1] = acc[h * rw : (h + 1) * rw].astype(bf)
        pre_copy(j).start()

    x_local(3, mine(2), NW - 1).start()
    for j in range(NC):
        if j == 1:
            x_remote(0, 2, 1).start()
        w_remote(j).start()
    for wv in range(2, NW):
        x_remote(0, 2, wv).start()
    for wv in range(NW):
        for D in range(2):
            x_remote(1 + D, NEAR[D], wv).start()
    for wv in range(NW):
        x_remote(3, 0, wv).start()

    @pl.loop(1, NC)
    def _(j):
        acc = half_product(0, w_own, j)
        pre_copy(j).wait_recv()
        for D in range(2):
            part = acc[D * rw : (D + 1) * rw] + pre[j, D].astype(jnp.float32)
            stage[D, j, 0] = part.astype(bf)
            far_copy(D, j, 0, j).start()

    x_local(0, mine(NEAR[0]), 0).start()
    remote(pre, pre, pre_send, pre_recv.at[0], partner).wait_send()

    @pl.loop(1, NW)
    def _(wv):
        x_local(wv, mine(2), wv).wait()
        x_landed(wv - 1, 1, wv - 1).wait_recv()

        @pl.when(wv == 1)
        def _():
            remote(w_par, w_par, wx_send, wx_recv, partner).wait_recv()

        @pl.loop(0, NC)
        def _(j):
            slot = j

            acc = product(wv, wv - 1, j)
            for D in range(2):
                far_copy(D, slot, wv, j).wait_send()
                stage[D, slot, 0] = acc[D * rw : (D + 1) * rw].astype(bf)
                far_copy(D, slot, wv, j).start()

        D = lax.rem(wv, 2)
        x_local(wv, mine(1 + 2 * D), lax.div(wv, 2)).start()

    x_landed(NW - 1, 2 * NW, NW - 1).wait_recv()

    @pl.loop(0, NW)
    def _(wv):
        t0 = lax.rem(2 * wv, 4)
        for D in range(2):
            x_local(t0 + D, mine(NEAR[D]), wv).wait()
            far_landed(D, wv).wait_recv()

        @pl.loop(0, NC)
        def _(j):
            slot = j
            for D in range(2):
                acc = product(t0 + D, (1 + D) * NW - 1 + wv, j)

                @pl.when(wv == 0)
                def _():
                    far_copy(D, slot, wv, j).wait_send()

                @pl.when(wv > 0)
                def _():
                    near_copy(D, slot, wv, j).wait_send()

                for h in range(2):
                    part = acc[h * rw : (h + 1) * rw]
                    if h == D:
                        part = part + far[D, wv, j].astype(jnp.float32)
                    stage[D, slot, h] = part.astype(bf)
                near_copy(D, slot, wv, j).start()

        for D in range(2):

            @pl.when(wv < 2)
            def _():
                x_local(t0 + D, mine(NEAR[D]), wv + 2).start()

            @pl.when(wv >= 2)
            def _():
                x_local(t0 + D, mine(0), 2 * (wv - 2) + D).start()

    pltpu.make_async_copy(g, gv, g_sem).wait()
    gain = gv[...].astype(jnp.float32).reshape(1, hid)
    x_landed(3 * NW - 1, NW, NW).wait_recv()

    @pl.loop(0, NW)
    def _(wv):
        x_local(wv, mine(0), wv).wait()
        for D in range(2):
            near_landed(D, wv).wait_recv()

        @pl.loop(0, NC)
        def _(j):
            acc = product(wv, 3 * NW - 1 + wv, j)
            for h in range(2):
                y = acc[h * rw : (h + 1) * rw]
                y = y + z[mine(0), h, wave(wv), cols(j)].astype(jnp.float32)
                y = y + near1[wv, h, :, cols(j)].astype(jnp.float32)
                z[mine(0), h, wave(wv), cols(j)] = y.astype(bf)

        for h in range(2):
            r_local(wv, h).wait()

            @pl.loop(0, rw // 16)
            def _(i):
                q = pl.ds(pl.multiple_of(i * 16, 16), 16)
                p = pl.ds(pl.multiple_of(wv * rw + i * 16, 16), 16)
                a = rt[h, q].astype(jnp.float32) + z[mine(0), h, p].astype(jnp.float32)
                ms = jnp.mean(a * a, axis=-1, keepdims=True)
                z[mine(0), h, p] = (a * lax.rsqrt(ms + EPS) * gain).astype(bf)

            for D in range(2):
                own_copy(D, wv, h).start()
            d2d(z.at[mine(0), h, wave(wv)], 0).start()

            @pl.when(wv < NW - 1)
            def _():
                r_local(wv + 1, h).start()

    for wv in range(NW):
        for h in range(2):
            for D in range(2):
                ag_landed(D, wv, h).wait_recv()
                for n, (lo, hi) in enumerate(ranges):
                    if h == D and lo // rw == wv:
                        fwd_copy(D, n).start()
                d2d(z.at[mine(4 - NEAR[D]), h, wave(wv)], 1).start()

    def swapped(q, like):
        d2d(like, q).wait_send()
        d2d(like, q).wait_recv()

    swapped(1, z.at[pl.ds(0, 2)])

    @pl.when(k == 1)
    def _():
        for D in range(2):
            for i in range(2):
                last_copy(D, i).start()

    for D in range(2):

        @pl.when(k == D)
        def _():
            for i in range(2):
                for copy in late_local(D, i):
                    copy.start()

    @pl.loop(0, SLOTS)
    def _(slot):
        for D in range(2):
            near_copy(D, slot, 0, 0).wait_send()

    remote(xp, xp, xp_send, xp_recv.at[0], partner).wait_send()
    remote(w_par, w_par, wx_send, wx_recv, partner).wait_send()
    v = z.at[pl.ds(0, 2)]
    remote(v, v, own_send, ag_recv.at[0, 0, 0], partner).wait_send()
    swapped(0, z.at[0])
    for n, v in enumerate((late_a1, late_a2, late_b)):
        pltpu.make_async_copy(v, v, late_sem.at[n]).wait()

    for n, (lo, hi) in enumerate(ranges):
        for D in range(2):
            fwd_copy(D, n).wait_recv()
            d2d(z.at[mine(2), D, pl.ds(lo, hi - lo)], 2).start()
    v = z.at[0, :, pl.ds(0, R0)]
    remote(v, v, fwd_send, fwd_recv.at[0, 0], partner).wait_send()
    swapped(2, v)

    @pl.when(k == 1)
    def _():
        remote(last, last, last_send, last_recv, to[0]).wait()


def store_kernel(z, o, sem):
    n = z.shape[0]
    for i in range(n):
        pltpu.make_async_copy(z.at[i], o.at[i], sem.at[i]).start()
    for i in range(n):
        pltpu.make_async_copy(z.at[i], o.at[i], sem.at[i]).wait()


def place(copies):
    for copy in copies:
        copy.start()
    for copy in copies:
        copy.wait()


def across():
    me = lax.axis_index("tp")
    return lax.rem(me, 2), lax.rem(lax.div(me, 2) + 2, CHIPS) * 2


def rows_of(o, b, h, lo, hi):
    return o.at[b, h, pl.ds(lo, hi - lo)]


def last_kernel(o_in, late_a1, last, last_other, o, sem):
    k, chip = across()
    rest = [(late_a1.at[i], rows_of(o, chip + i, k, R2, R3)) for i in range(2)]
    for core, v in enumerate((last_other, last)):

        @pl.when(k == core)
        def _():
            pairs = rest + [
                (v.at[i, D], rows_of(o, chip + i, D, R0, R1)) for i in range(2) for D in range(2)
            ]
            place([pltpu.make_async_copy(*p, sem.at[n]) for n, p in enumerate(pairs)])


def middle_kernel(o_in, late_b, late_a1_other, o, sem):
    k, chip = across()
    pairs = []
    for i in range(2):
        pairs.append((late_b.at[i], rows_of(o, chip + i, 1 - k, R1, R2)))
        pairs.append((late_a1_other.at[i], rows_of(o, chip + i, 1 - k, R2, R3)))
    place([pltpu.make_async_copy(*p, sem.at[n]) for n, p in enumerate(pairs)])


def late_kernel(o_in, late_a2, late_b_other, late_a2_other, o, sem):
    k, chip = across()
    half = o.shape[2]
    pairs = []
    for i in range(2):
        pairs.append((late_a2.at[i], rows_of(o, chip + i, k, R3, half)))
        pairs.append((late_b_other.at[i], rows_of(o, chip + i, k, R1, R2)))
        pairs.append((late_a2_other.at[i], rows_of(o, chip + i, 1 - k, R3, half)))
    place([pltpu.make_async_copy(*p, sem.at[n]) for n, p in enumerate(pairs)])


def solution(mesh):
    tp = mesh.shape["tp"]
    onward = [(i, (i + 2 if i % 2 == 0 else i - 2) % tp) for i in range(tp)]
    back = [(i, (i - 2 if i % 2 == 0 else i + 2) % tp) for i in range(tp)]
    swap = [(i, i + 1 - 2 * (i % 2)) for i in range(tp)]

    def body(x, w, r, g):
        t, kd = x.shape
        hid = w.shape[1]
        half = t // tp // 2
        rw, cw = half // NW, hid // NC
        x5 = x.reshape(tp, 2, NW, rw, kd)
        r5 = r.reshape(tp, 2, NW, rw, hid)
        dma = pltpu.SemaphoreType.DMA
        bf = jnp.bfloat16
        any_spec = pl.BlockSpec(memory_space=pl.ANY)
        z, late_a1, late_a2, late_b, last = pl.pallas_call(
            ring_kernel,
            name="ring",
            out_shape=(
                pltpu.VMEM((tp, 2, half, hid), bf),
                jax.ShapeDtypeStruct((2, R3 - R2, hid), bf),
                jax.ShapeDtypeStruct((2, half - R3, hid), bf),
                jax.ShapeDtypeStruct((2, R2 - R1, hid), bf),
                jax.ShapeDtypeStruct((2, 2, R1 - R0, hid), bf),
            ),
            in_specs=[any_spec] * 4,
            out_specs=(pl.BlockSpec(memory_space=pltpu.VMEM),) + (any_spec,) * 4,
            scratch_shapes=[
                pltpu.VMEM((hid,), bf),
                pltpu.VMEM((NC, kd, cw), bf),
                pltpu.VMEM((NC, kd, cw), bf),
                pltpu.VMEM((4, 2, rw, kd), bf),
                pltpu.VMEM((4 * NW - 1, 2, rw, kd), bf),
                pltpu.VMEM((NC, 2, rw, cw), bf),
                pltpu.VMEM((2, NW, NC, rw, cw), bf),
                pltpu.VMEM((NW, 2, rw, hid), bf),
                pltpu.VMEM((2, SLOTS, 2, rw, cw), bf),
                pltpu.VMEM((2, rw, hid), bf),
                dma, dma((NC + 1,)), dma((4,)), dma((2,)), dma((3,)),
                dma, dma, dma, dma((NW + 1,)), dma, dma((NC + 1,)),
                dma((2, SLOTS)), dma((2, NW)), dma((2, NW)),
                dma, dma((2, NW, 2)), dma, dma((2, -(-R0 // STEP))), dma, dma, dma((3,)), dma((3,)),
            ],
            compiler_params=pltpu.CompilerParams(
                collective_id=0, has_side_effects=True, vmem_limit_bytes=33000000
            ),
        )(x5, w, r5, g)
        late_a1 = lax.ppermute(late_a1, "tp", onward)
        late_b = lax.ppermute(late_b, "tp", back)
        late_a2 = lax.ppermute(late_a2, "tp", onward)
        last_other = lax.ppermute(last, "tp", swap)
        out = pl.pallas_call(
            store_kernel,
            name="store",
            out_shape=jax.ShapeDtypeStruct(z.shape, bf),
            in_specs=[pl.BlockSpec(memory_space=pltpu.VMEM)],
            out_specs=any_spec,
            scratch_shapes=[dma((tp,))],
            compiler_params=pltpu.CompilerParams(vmem_limit_bytes=1 << 20),
            cost_estimate=pl.CostEstimate(
                flops=10**10, bytes_accessed=2 * t * hid, transcendentals=0
            ),
        )(z)
        out, late_a1, last_other = lax.optimization_barrier((out, late_a1, last_other))
        late_a1_other = lax.ppermute(late_a1, "tp", swap)

        def in_place(kernel, *args):
            return pl.pallas_call(
                kernel,
                out_shape=jax.ShapeDtypeStruct(z.shape, bf),
                in_specs=[any_spec] * len(args),
                out_specs=any_spec,
                scratch_shapes=[dma((6,))],
                input_output_aliases={0: 0},
                compiler_params=pltpu.CompilerParams(vmem_limit_bytes=1 << 20),
                cost_estimate=pl.CostEstimate(
                    flops=10**9, bytes_accessed=t * hid // 4, transcendentals=0
                ),
            )(*args)

        out = in_place(last_kernel, out, late_a1, last, last_other)
        out, late_b, late_a2 = lax.optimization_barrier((out, late_b, late_a2))
        late_b_other = lax.ppermute(late_b, "tp", swap)
        late_a2_other = lax.ppermute(late_a2, "tp", swap)
        out = in_place(middle_kernel, out, late_b, late_a1_other)
        out = in_place(late_kernel, out, late_a2, late_b_other, late_a2_other)
        return out.reshape(t, hid)

    return jax.shard_map(
        body,
        mesh=mesh,
        in_specs=(P("data", "tp"), P("tp", None), P("data", None), P(None)),
        out_specs=P("data", None),
        check_vma=False,
    )
```

```python
import jax
import jax.numpy as jnp
from jax import lax
from jax.experimental import pallas as pl
from jax.experimental.pallas import tpu as pltpu
from jax.sharding import PartitionSpec as P


EPS = 1e-6
MESH = pl.DeviceIdType.MESH
CHIPS = 4
NW = 4
NC = 4
R0, R1, R2, R3 = 192, 288, 368, 496
STEP = 32
SLOTS = 4
FIRST = 128
NEAR = (1, 3)


def ring_kernel(
    x, w, r, g, z, late_a1, late_a2, late_b, last,
    gv, w_own, w_par, xt, xp, pre, far, near1, stage, rt,
    g_sem, w_sem, xt_sem, rt_sem, late_sem,
    wx_send, wx_recv, xp_send, xp_recv, pre_send, pre_recv,
    st_send, far_recv, near_recv,
    own_send, ag_recv, fwd_send, fwd_recv, last_send, last_recv, d_send, d_recv,
):
    me = lax.axis_index("tp")
    k = lax.rem(me, 2)
    c = lax.div(me, 2)
    chip = lambda d: lax.rem(c + d, CHIPS)
    mine = lambda d: chip(d) * 2 + k
    other = lambda d: chip(d) * 2 + 1 - k
    partner = c * 2 + 1 - k
    to = (mine(1), mine(3))
    rw, kd = x.shape[3], x.shape[4]
    half = NW * rw
    ranges = [(lo, min(lo + STEP, R0)) for lo in range(0, R0, STEP)]
    hid = w.shape[1]
    cw = hid // NC
    bf = jnp.bfloat16

    def remote(src, dst, ssem, rsem, dev):
        return pltpu.make_async_remote_copy(
            src_ref=src, dst_ref=dst, send_sem=ssem, recv_sem=rsem,
            device_id={"tp": dev}, device_id_type=MESH,
        )

    def cols(j):
        return pl.ds(pl.multiple_of(j * cw, cw), cw)

    def wave(wv):
        return pl.ds(pl.multiple_of(wv * rw, rw), rw)

    def w_local(j):
        return pltpu.make_async_copy(w.at[:, cols(j)], w_own.at[j], w_sem.at[j])

    def w_local_part(lo, hi, q):
        v = pl.ds(lo, hi - lo)
        return pltpu.make_async_copy(w.at[:, v], w_own.at[0, :, v], w_sem.at[q])

    def w_remote(j):
        return remote(w.at[:, cols(j)], w_par.at[j], wx_send, wx_recv, partner)

    def x_local(t, b, wv):
        return pltpu.make_async_copy(x.at[b, :, wv], xt.at[t], xt_sem.at[t])

    def x_remote(e, d, wv):
        q = wv - 1 if e == 0 else (NW - 1 if e < 3 else NW)
        return remote(x.at[other(d), :, wv], xp.at[e * NW + wv - 1], xp_send, xp_recv.at[q], partner)

    def x_landed(first, n, q):
        v = xp.at[pl.ds(first, n)]
        return remote(v, v, xp_send, xp_recv.at[q], partner)

    def pre_copy(j):
        return remote(stage.at[:, j, 1], pre.at[j], pre_send, pre_recv.at[j], partner)

    def pre_part(lo, hi, q):
        v = pl.ds(lo, hi - lo)
        return remote(stage.at[:, 0, 1, :, v], pre.at[0, :, :, v], pre_send, pre_recv.at[q], partner)

    def r_local(wv, h):
        return pltpu.make_async_copy(r.at[mine(0), h, wv], rt.at[h], rt_sem.at[h])

    def far_copy(D, slot, wv, j):
        return remote(
            stage.at[D, slot, 0], far.at[D, wv, j],
            st_send.at[D, slot], far_recv.at[wv], to[D],
        )

    def far_part(D, lo, hi):
        v = pl.ds(lo, hi - lo)
        sems = st_send.at[D, 0], far_recv.at[0]
        return remote(stage.at[D, 0, 0, :, v], far.at[D, 0, 0, :, v], *sems, to[D])

    def far_landed(wv):
        v = far.at[:, wv]
        return remote(v, v, st_send.at[0, 0], far_recv.at[wv], to[0])

    def near_copy(D, slot, wv, j):
        dst = z.at[to[0], :, wave(wv), cols(j)] if D == 0 else near1.at[wv, :, :, cols(j)]
        return remote(stage.at[D, slot], dst, st_send.at[D, slot], near_recv.at[wv], to[D])

    def near_landed(wv):
        v = near1.at[pl.ds(0, 2)]
        return remote(v, v, st_send.at[0, 0], near_recv.at[wv], to[0])

    def own_copy(D, wv, h):
        v = z.at[mine(0), h, wave(wv)]
        return remote(v, v, own_send, ag_recv.at[wv, h], to[D])

    def ag_landed(wv, h):
        v = z.at[0, :, wave(wv)]
        return remote(v, v, own_send, ag_recv.at[wv, h], to[0])

    def fwd_copy(D, n):
        lo, hi = ranges[n]
        v = z.at[mine(4 - NEAR[D]), D, pl.ds(lo, hi - lo)]
        return remote(v, v, fwd_send, fwd_recv.at[D, n], to[D])

    def last_copy(D, i):
        v = z.at[chip(4 - NEAR[D]) * 2 + i, D, pl.ds(R0, R1 - R0)]
        return remote(v, last.at[i, D], last_send, last_recv, to[D])

    def d2d(v, q):
        return remote(v, v, d_send.at[q], d_recv.at[q], partner)

    def late_local(D, i):
        src = lambda D, lo, hi: z.at[chip(4 - NEAR[D]) * 2 + i, D, pl.ds(lo, hi - lo)]
        return (
            pltpu.make_async_copy(src(D, R2, R3), late_a1.at[i], late_sem.at[0]),
            pltpu.make_async_copy(src(D, R3, half), late_a2.at[i], late_sem.at[1]),
            pltpu.make_async_copy(src(1 - D, R1, R2), late_b.at[i], late_sem.at[2]),
        )

    def half_product(t, ww, j):
        return jnp.dot(xt[t].reshape(2 * rw, kd), ww[j], preferred_element_type=jnp.float32)

    def part_product(t, lo, hi):
        a = xt[t].reshape(2 * rw, kd)
        return jnp.dot(a, w_own[0, :, lo:hi], preferred_element_type=jnp.float32)

    def product(t, p, j):
        b = xp[p].reshape(2 * rw, kd)
        return half_product(t, w_own, j) + jnp.dot(b, w_par[j], preferred_element_type=jnp.float32)

    parts = (0, FIRST, 0), (FIRST, cw, NC)
    barrier = pltpu.get_barrier_semaphore()
    for dev in (partner, to[0], to[1]):
        pl.semaphore_signal(barrier, inc=1, device_id={"tp": dev}, device_id_type=MESH)
    x_local(3, other(2), 0).start()
    for part in parts:
        w_local_part(*part).start()
    x_local(0, mine(2), 0).start()
    for j in range(1, NC):
        w_local(j).start()
    for wv in range(1, NW - 1):
        x_local(wv, mine(2), wv).start()
    for h in range(2):
        r_local(0, h).start()
    pltpu.make_async_copy(g, gv, g_sem).start()

    x_local(3, other(2), 0).wait()

    for lo, hi, q in parts:
        w_local_part(lo, hi, q).wait()
        acc = part_product(3, lo, hi)
        for h in range(2):
            stage[h, 0, 1, :, lo:hi] = acc[h * rw : (h + 1) * rw].astype(bf)
        if lo == 0:
            pl.semaphore_wait(barrier, 3)
        pre_part(lo, hi, q).start()

    x_local(0, mine(2), 0).wait()

    for lo, hi, q in parts:
        acc = part_product(0, lo, hi)
        pre_part(lo, hi, q).wait_recv()
        for D in range(2):
            part = acc[D * rw : (D + 1) * rw] + pre[0, D, :, lo:hi].astype(jnp.float32)
            stage[D, 0, 0, :, lo:hi] = part.astype(bf)
            far_part(D, lo, hi).start()

    @pl.loop(1, NC)
    def _(j):
        w_local(j).wait()
        acc = half_product(3, w_own, j)
        for h in range(2):
            stage[h, j, 1] = acc[h * rw : (h + 1) * rw].astype(bf)
        pre_copy(j).start()

    def first_wave(j):
        acc = half_product(0, w_own, j)
        pre_copy(j).wait_recv()
        for D in range(2):
            part = acc[D * rw : (D + 1) * rw] + pre[j, D].astype(jnp.float32)
            stage[D, j, 0] = part.astype(bf)
            far_copy(D, j, 0, j).start()

    first_wave(1)

    x_local(3, mine(2), NW - 1).start()
    for j in range(NC):
        if j == 1:
            x_remote(0, 2, 1).start()
        w_remote(j).start()
    for wv in range(2, NW):
        x_remote(0, 2, wv).start()
    for wv in range(NW):
        for D in range(2):
            x_remote(1 + D, NEAR[D], wv).start()
    for wv in range(NW):
        x_remote(3, 0, wv).start()

    pl.loop(2, NC)(first_wave)
    x_local(0, mine(NEAR[0]), 0).start()
    remote(pre, pre, pre_send, pre_recv.at[0], partner).wait_send()

    @pl.loop(1, NW)
    def _(wv):
        x_local(wv, mine(2), wv).wait()
        x_landed(wv - 1, 1, wv - 1).wait_recv()

        @pl.when(wv == 1)
        def _():
            remote(w_par, w_par, wx_send, wx_recv, partner).wait_recv()

        @pl.loop(0, NC)
        def _(j):
            slot = j

            acc = product(wv, wv - 1, j)
            for D in range(2):
                far_copy(D, slot, wv, j).wait_send()
                stage[D, slot, 0] = acc[D * rw : (D + 1) * rw].astype(bf)
                far_copy(D, slot, wv, j).start()

        D = lax.rem(wv, 2)
        x_local(wv, mine(1 + 2 * D), lax.div(wv, 2)).start()

    x_landed(NW - 1, 2 * NW, NW - 1).wait_recv()

    @pl.loop(0, NW)
    def _(wv):
        t0 = lax.rem(2 * wv, 4)
        for D in range(2):
            x_local(t0 + D, mine(NEAR[D]), wv).wait()
        far_landed(wv).wait_recv()

        @pl.loop(0, NC)
        def _(j):
            slot = j
            for D in range(2):
                acc = product(t0 + D, (1 + D) * NW - 1 + wv, j)

                @pl.when(wv == 0)
                def _():
                    far_copy(D, slot, wv, j).wait_send()

                @pl.when(wv > 0)
                def _():
                    near_copy(D, slot, wv, j).wait_send()

                for h in range(2):
                    part = acc[h * rw : (h + 1) * rw]
                    if h == D:
                        part = part + far[D, wv, j].astype(jnp.float32)
                    stage[D, slot, h] = part.astype(bf)
                near_copy(D, slot, wv, j).start()

        for D in range(2):

            @pl.when(wv < 2)
            def _():
                x_local(t0 + D, mine(NEAR[D]), wv + 2).start()

            @pl.when(wv >= 2)
            def _():
                x_local(t0 + D, mine(0), 2 * (wv - 2) + D).start()

    pltpu.make_async_copy(g, gv, g_sem).wait()
    gain = gv[...].astype(jnp.float32).reshape(1, hid)
    x_landed(3 * NW - 1, NW, NW).wait_recv()

    @pl.loop(0, NW)
    def _(wv):
        x_local(wv, mine(0), wv).wait()
        near_landed(wv).wait_recv()

        @pl.loop(0, NC)
        def _(j):
            acc = product(wv, 3 * NW - 1 + wv, j)
            for h in range(2):
                y = acc[h * rw : (h + 1) * rw]
                y = y + z[mine(0), h, wave(wv), cols(j)].astype(jnp.float32)
                y = y + near1[wv, h, :, cols(j)].astype(jnp.float32)
                z[mine(0), h, wave(wv), cols(j)] = y.astype(bf)

        for h in range(2):
            r_local(wv, h).wait()

            @pl.loop(0, rw // 16)
            def _(i):
                q = pl.ds(pl.multiple_of(i * 16, 16), 16)
                p = pl.ds(pl.multiple_of(wv * rw + i * 16, 16), 16)
                a = rt[h, q].astype(jnp.float32) + z[mine(0), h, p].astype(jnp.float32)
                ms = jnp.mean(a * a, axis=-1, keepdims=True)
                z[mine(0), h, p] = (a * lax.rsqrt(ms + EPS) * gain).astype(bf)

            for D in range(2):
                own_copy(D, wv, h).start()
            d2d(z.at[mine(0), h, wave(wv)], 0).start()

            @pl.when(wv < NW - 1)
            def _():
                r_local(wv + 1, h).start()

    for wv in range(NW):
        for h in range(2):
            ag_landed(wv, h).wait_recv()
            for D in range(2):
                for n, (lo, hi) in enumerate(ranges):
                    if h == D and lo // rw == wv:
                        fwd_copy(D, n).start()
                d2d(z.at[mine(4 - NEAR[D]), h, wave(wv)], 1).start()

    def swapped(q, like):
        d2d(like, q).wait_send()
        d2d(like, q).wait_recv()

    swapped(1, z.at[pl.ds(0, 2)])

    @pl.when(k == 1)
    def _():
        for D in range(2):
            for i in range(2):
                last_copy(D, i).start()

    for D in range(2):

        @pl.when(k == D)
        def _():
            for i in range(2):
                for copy in late_local(D, i):
                    copy.start()

    @pl.loop(0, SLOTS)
    def _(slot):
        for D in range(2):
            near_copy(D, slot, 0, 0).wait_send()

    remote(xp, xp, xp_send, xp_recv.at[0], partner).wait_send()
    remote(w_par, w_par, wx_send, wx_recv, partner).wait_send()
    v = z.at[pl.ds(0, 2)]
    remote(v, v, own_send, ag_recv.at[0, 0], partner).wait_send()
    swapped(0, z.at[0])
    for n, v in enumerate((late_a1, late_a2, late_b)):
        pltpu.make_async_copy(v, v, late_sem.at[n]).wait()

    for n, (lo, hi) in enumerate(ranges):
        for D in range(2):
            fwd_copy(D, n).wait_recv()
            d2d(z.at[mine(2), D, pl.ds(lo, hi - lo)], 2).start()
    v = z.at[0, :, pl.ds(0, R0)]
    remote(v, v, fwd_send, fwd_recv.at[0, 0], partner).wait_send()
    swapped(2, v)

    @pl.when(k == 1)
    def _():
        remote(last, last, last_send, last_recv, to[0]).wait()


def store_kernel(z, o, sem):
    n = z.shape[0]
    for i in range(n):
        pltpu.make_async_copy(z.at[i], o.at[i], sem.at[i]).start()
    for i in range(n):
        pltpu.make_async_copy(z.at[i], o.at[i], sem.at[i]).wait()


def place(copies):
    for copy in copies:
        copy.start()
    for copy in copies:
        copy.wait()


def across():
    me = lax.axis_index("tp")
    return lax.rem(me, 2), lax.rem(lax.div(me, 2) + 2, CHIPS) * 2


def rows_of(o, b, h, lo, hi):
    return o.at[b, h, pl.ds(lo, hi - lo)]


def last_kernel(o_in, late_a1, last, last_other, o, sem):
    k, chip = across()
    rest = [(late_a1.at[i], rows_of(o, chip + i, k, R2, R3)) for i in range(2)]
    for core, v in enumerate((last_other, last)):

        @pl.when(k == core)
        def _():
            pairs = rest + [
                (v.at[i, D], rows_of(o, chip + i, D, R0, R1)) for i in range(2) for D in range(2)
            ]
            place([pltpu.make_async_copy(*p, sem.at[n]) for n, p in enumerate(pairs)])


def middle_kernel(o_in, late_b, late_a1_other, late_a2, o, sem):
    k, chip = across()
    pairs = []
    for i in range(2):
        pairs.append((late_b.at[i], rows_of(o, chip + i, 1 - k, R1, R2)))
        pairs.append((late_a1_other.at[i], rows_of(o, chip + i, 1 - k, R2, R3)))
        pairs.append((late_a2.at[i], rows_of(o, chip + i, k, R3, o.shape[2])))
    place([pltpu.make_async_copy(*p, sem.at[n]) for n, p in enumerate(pairs)])


def late_kernel(o_in, late_b_other, late_a2_other, o, sem):
    k, chip = across()
    half = o.shape[2]
    pairs = []
    for i in range(2):
        pairs.append((late_b_other.at[i], rows_of(o, chip + i, k, R1, R2)))
        pairs.append((late_a2_other.at[i], rows_of(o, chip + i, 1 - k, R3, half)))
    place([pltpu.make_async_copy(*p, sem.at[n]) for n, p in enumerate(pairs)])


def solution(mesh):
    tp = mesh.shape["tp"]
    onward = [(i, (i + 2 if i % 2 == 0 else i - 2) % tp) for i in range(tp)]
    back = [(i, (i - 2 if i % 2 == 0 else i + 2) % tp) for i in range(tp)]
    swap = [(i, i + 1 - 2 * (i % 2)) for i in range(tp)]

    def body(x, w, r, g):
        t, kd = x.shape
        hid = w.shape[1]
        half = t // tp // 2
        rw, cw = half // NW, hid // NC
        x5 = x.reshape(tp, 2, NW, rw, kd)
        r5 = r.reshape(tp, 2, NW, rw, hid)
        dma = pltpu.SemaphoreType.DMA
        bf = jnp.bfloat16
        any_spec = pl.BlockSpec(memory_space=pl.ANY)
        z, late_a1, late_a2, late_b, last = pl.pallas_call(
            ring_kernel,
            name="ring",
            out_shape=(
                pltpu.VMEM((tp, 2, half, hid), bf),
                jax.ShapeDtypeStruct((2, R3 - R2, hid), bf),
                jax.ShapeDtypeStruct((2, half - R3, hid), bf),
                jax.ShapeDtypeStruct((2, R2 - R1, hid), bf),
                jax.ShapeDtypeStruct((2, 2, R1 - R0, hid), bf),
            ),
            in_specs=[any_spec] * 4,
            out_specs=(pl.BlockSpec(memory_space=pltpu.VMEM),) + (any_spec,) * 4,
            scratch_shapes=[
                pltpu.VMEM((hid,), bf),
                pltpu.VMEM((NC, kd, cw), bf),
                pltpu.VMEM((NC, kd, cw), bf),
                pltpu.VMEM((4, 2, rw, kd), bf),
                pltpu.VMEM((4 * NW - 1, 2, rw, kd), bf),
                pltpu.VMEM((NC, 2, rw, cw), bf),
                pltpu.VMEM((2, NW, NC, rw, cw), bf),
                pltpu.VMEM((NW, 2, rw, hid), bf),
                pltpu.VMEM((2, SLOTS, 2, rw, cw), bf),
                pltpu.VMEM((2, rw, hid), bf),
                dma, dma((NC + 1,)), dma((4,)), dma((2,)), dma((3,)),
                dma, dma, dma, dma((NW + 1,)), dma, dma((NC + 1,)),
                dma((2, SLOTS)), dma((NW,)), dma((NW,)),
                dma, dma((NW, 2)), dma, dma((2, -(-R0 // STEP))), dma, dma, dma((3,)), dma((3,)),
            ],
            compiler_params=pltpu.CompilerParams(
                collective_id=0, has_side_effects=True, vmem_limit_bytes=33000000
            ),
        )(x5, w, r5, g)
        late_a1 = lax.ppermute(late_a1, "tp", onward)
        late_b = lax.ppermute(late_b, "tp", back)
        late_a2 = lax.ppermute(late_a2, "tp", onward)
        last_other = lax.ppermute(last, "tp", swap)
        out = pl.pallas_call(
            store_kernel,
            name="store",
            out_shape=jax.ShapeDtypeStruct(z.shape, bf),
            in_specs=[pl.BlockSpec(memory_space=pltpu.VMEM)],
            out_specs=any_spec,
            scratch_shapes=[dma((tp,))],
            compiler_params=pltpu.CompilerParams(vmem_limit_bytes=1 << 20),
            cost_estimate=pl.CostEstimate(
                flops=10**10, bytes_accessed=2 * t * hid, transcendentals=0
            ),
        )(z)
        out, late_a1, last_other = lax.optimization_barrier((out, late_a1, last_other))
        late_a1_other = lax.ppermute(late_a1, "tp", swap)

        def in_place(kernel, *args):
            return pl.pallas_call(
                kernel,
                out_shape=jax.ShapeDtypeStruct(z.shape, bf),
                in_specs=[any_spec] * len(args),
                out_specs=any_spec,
                scratch_shapes=[dma((6,))],
                input_output_aliases={0: 0},
                compiler_params=pltpu.CompilerParams(vmem_limit_bytes=1 << 20),
                cost_estimate=pl.CostEstimate(
                    flops=10**9, bytes_accessed=t * hid // 4, transcendentals=0
                ),
            )(*args)

        out = in_place(last_kernel, out, late_a1, last, last_other)
        out, late_b, late_a2 = lax.optimization_barrier((out, late_b, late_a2))
        late_b_other = lax.ppermute(late_b, "tp", swap)
        late_a2_other = lax.ppermute(late_a2, "tp", swap)
        out = in_place(middle_kernel, out, late_b, late_a1_other, late_a2)
        out = in_place(late_kernel, out, late_b_other, late_a2_other)
        return out.reshape(t, hid)

    return jax.shard_map(
        body,
        mesh=mesh,
        in_specs=(P("data", "tp"), P("tp", None), P("data", None), P(None)),
        out_specs=P("data", None),
        check_vma=False,
    )
```
